256 devices in a mesh: band: 64 (over y, z, core), feat: 4 (over x).
Axes of the slice: x: 4, y: 4, z: 8, core: 2. Of those that a mesh axis runs over, the one named last changes fastest.
Arguments:
- grid_latent: bfloat16 [131072, 512], P('band', 'feat'), may hold values from -6 to 6
- mesh_latent: bfloat16 [10240, 512], P('band', 'feat'), may hold values from -6 to 6
- edge_latent: bfloat16 [64, 4, 2048, 512], P('band', 'feat'), may hold values from -6 to 6
- edge_src: int32 [64, 8192], P('band'), may hold values from 0 to 2047
- edge_dst: int32 [64, 4, 2048], P('band', 'feat'), may hold values from 0 to 160, as said below
- edge_w1: bfloat16 [1536, 512], replicated, may hold values from -0.15625 to 0.15625
- edge_b1: float32 [512], replicated, may hold values from -3 to 3
- edge_w2: bfloat16 [512, 512], replicated, may hold values from -0.25 to 0.25
- edge_b2: float32 [512], replicated, may hold values from -2 to 2
- edge_gain: float32 [512], replicated, may hold values from 0.25 to 1.75
- edge_shift: float32 [512], replicated, may hold values from -2 to 2
- node_w1: bfloat16 [1024, 512], replicated, may hold values from -0.1875 to 0.1875
- node_b1: float32 [512], replicated, may hold values from -3 to 3
- node_w2: bfloat16 [512, 512], replicated, may hold values from -0.25 to 0.25
- node_b2: float32 [512], replicated, may hold values from -2 to 2
- node_gain: float32 [512], replicated, may hold values from 0.25 to 1.75
- node_shift: float32 [512], replicated, may hold values from -2 to 2
Outputs:
- mesh_new: bfloat16 [10240, 512], P('band', 'feat')
The draws below stay inside these ranges and needn't reach their ends.
Inputs may be any that keep to these rules, and one draw needn't show every extreme that they name: `edge_src`: entry [s, d * 128 + j] is the grid row, counted within band index s, that sends slot j of the edges from band index s to band index d; empty slots hold some row too. `edge_dst`: entry [d, f, s * 32 + q] is the mesh node, counted within band index d, that receives slot f * 32 + q of the edges from band index s to band index d, or 160 where that slot is empty. The used slots of a pair come first; a pair has at most 128 used slots. Each receiving band index d hears only from the sending band indices of one latitude span of consecutive indices (edges are local), which lies anywhere along band since mesh partitions are face-major; other pairs are empty. In every draw some band indices receive 128 from every band index of their span.
All inputs are finite; a program needn't handle non-finite values.
Results may differ from the reference program's by a relative error of at most 0.011.
Values may be sent and summed in bfloat16 or wider, within the bound.
No kernel may reach another device: no remote copies, remote signals or barrier semaphores. Data moves between devices by JAX's collectives and lax.ppermute only.
A program may use at most 64 MiB of HBM per device.

```python
import jax
import jax.numpy as jnp
from jax import lax

D = 512
H = 512
G_DEV = 2048
M_DEV = 160
CAP = 128
QUART = 32
GRID = 131072
MESH = 10240
N_BAND = 64
N_FEAT = 4


def pair_counts(key):
    base_key = jax.random.fold_in(key, 7)
    count_key, crowd_key, forced_key, center_key, half_key = jax.random.split(base_key, 5)
    counts = jax.random.randint(count_key, (N_BAND, N_BAND), 1, CAP + 1)
    crowded = jax.random.randint(crowd_key, (N_BAND,), 0, 8) == 0
    forced = jax.random.randint(forced_key, (), 0, N_BAND)
    crowded = crowded | (jnp.arange(N_BAND) == forced)
    centers = jax.random.randint(center_key, (N_BAND,), 0, N_BAND)
    halves = jax.random.randint(half_key, (N_BAND,), 3, 9)
    senders = jnp.arange(N_BAND)[:, None]
    linked = jnp.abs(senders - centers[None, :]) <= halves[None, :]
    counts = jnp.where(crowded[None, :], CAP, counts)
    return jnp.where(linked, counts, 0)


def draw_edge_dst(key, part):
    counts = pair_counts(key)
    node_key = jax.random.fold_in(key, 21)
    first_key, hot_key, pick_key, use_key = jax.random.split(node_key, 4)
    shape = (N_BAND, N_FEAT, N_BAND, QUART)
    uniform_node = jax.random.randint(first_key, shape, 0, M_DEV)
    hot_nodes = jax.random.randint(hot_key, (N_BAND, 4), 0, M_DEV)
    picks = jax.random.randint(pick_key, shape, 0, 4)
    use_hot = jax.random.randint(use_key, shape, 0, 3) == 0
    chosen = jnp.sum(jnp.where(picks[..., None] == jnp.arange(4), hot_nodes[:, None, None, None, :], 0), -1)
    nodes_all = jnp.where(use_hot, chosen, uniform_node)
    slot_index = jnp.arange(N_FEAT)[None, :, None, None] * QUART + jnp.arange(QUART)[None, None, None, :]
    filled = slot_index < jnp.transpose(counts)[:, None, :, None]
    result = jnp.where(filled, nodes_all, M_DEV)
    return result.reshape(N_BAND, N_FEAT, N_BAND * QUART).astype(jnp.int32)


def place_ends(drawn, stream_key, least, high):
    shape = drawn.shape
    index_at = [jax.random.randint(jax.random.fold_in(stream_key, axis), (), 0, shape[axis]) for axis in range(len(shape))]
    drawn = drawn.at[tuple(index_at)].set(least)
    longest = shape.index(max(shape))
    index_at[longest] = (index_at[longest] + 1) % shape[longest]
    return drawn.at[tuple(index_at)].set(high)


def steps_of(own_key, shape, cuts, low, largest):
    def one(axis_at, blocks):
        heights = jax.random.uniform(jax.random.fold_in(jax.random.fold_in(own_key, 6), axis_at), (blocks,), jnp.float32, low / len(cuts), largest / len(cuts))
        return jnp.repeat(jnp.exp(heights), shape[axis_at] // blocks).reshape((-1,) + (1,) * (len(shape) - axis_at - 1))

    gain = one(*cuts[0])
    for cut in cuts[1:]:
        gain = gain * one(*cut)
    return gain


def noise(own_key, extent, deviation, most, cuts=(), held_as=jnp.bfloat16):
    factor_of = steps_of(own_key, extent, cuts, -0.22, 0.18) if cuts else 1.0
    array = jax.random.normal(own_key, extent, jnp.float32) * deviation * factor_of
    return jnp.minimum(jnp.maximum(array, -most), most).astype(held_as)


def setup_inputs(seed: int = 0) -> dict:
    streams_of = jax.random.split(jax.random.key(seed), 18)
    grid_latent = noise(streams_of[0], (GRID, D), 1.0, 6.0, ((0, 64), (1, 4)))
    mesh_latent = noise(streams_of[1], (MESH, D), 1.0, 6.0, ((0, 64), (1, 4)))
    edge_latent = noise(streams_of[2], (N_BAND, N_FEAT, N_BAND * QUART, D), 1.0, 6.0, ((0, 64), (1, 4)))
    edge_src = place_ends(jax.random.randint(streams_of[3], (N_BAND, N_BAND * CAP), 0, G_DEV), jax.random.fold_in(streams_of[3], 1), 0, G_DEV - 1).astype(jnp.int32)
    edge_dst = draw_edge_dst(jax.random.fold_in(streams_of[17], 71), 0)
    edge_w1 = noise(streams_of[5], (3 * D, H), (3 * D) ** -0.5, 0.15625)
    edge_b1 = noise(streams_of[6], (H,), 0.5, 3.0, (), jnp.float32)
    edge_w2 = noise(streams_of[7], (H, D), H ** -0.5, 0.25)
    edge_b2 = noise(streams_of[8], (D,), 0.3, 2.0, (), jnp.float32)
    edge_gain = jnp.clip(1.0 + 0.15 * jax.random.normal(streams_of[9], (D,), jnp.float32), 0.25, 1.75)
    edge_shift = noise(streams_of[10], (D,), 0.3, 2.0, (), jnp.float32)
    node_w1 = noise(streams_of[11], (2 * D, H), (2 * D) ** -0.5, 0.1875)
    node_b1 = noise(streams_of[12], (H,), 0.5, 3.0, (), jnp.float32)
    node_w2 = noise(streams_of[13], (H, D), H ** -0.5, 0.25)
    node_b2 = noise(streams_of[14], (D,), 0.3, 2.0, (), jnp.float32)
    node_gain = jnp.clip(1.0 + 0.15 * jax.random.normal(streams_of[15], (D,), jnp.float32), 0.25, 1.75)
    node_shift = noise(streams_of[16], (D,), 0.3, 2.0, (), jnp.float32)
    return {"grid_latent": grid_latent, "mesh_latent": mesh_latent, "edge_latent": edge_latent, "edge_src": edge_src, "edge_dst": edge_dst, "edge_w1": edge_w1, "edge_b1": edge_b1, "edge_w2": edge_w2, "edge_b2": edge_b2, "edge_gain": edge_gain, "edge_shift": edge_shift, "node_w1": node_w1, "node_b1": node_b1, "node_w2": node_w2, "node_b2": node_b2, "node_gain": node_gain, "node_shift": node_shift}


EPSILON = 1e-05

def normalize(values, norm_gain, norm_shift):
    average = lax.optimization_barrier(jnp.mean(values, -1, keepdims=True))
    centered = values - average
    variance = lax.optimization_barrier(jnp.mean(centered * centered, -1, keepdims=True))
    return centered * lax.rsqrt(variance + EPSILON) * norm_gain + norm_shift

def reference(grid_latent, mesh_latent, edge_latent, edge_src, edge_dst, edge_w1, edge_b1, edge_w2, edge_b2, edge_gain, edge_shift, node_w1, node_b1, node_w2, node_b2, node_gain, node_shift):
    full_width = grid_latent.shape[1]
    slot_count = N_FEAT * N_BAND * QUART
    local_src = edge_src.reshape(N_BAND, N_BAND, N_FEAT, QUART)
    offsets = (jnp.arange(N_BAND, dtype=jnp.int32) * G_DEV)[:, None, None, None]
    global_src = jnp.transpose(local_src + offsets, (1, 2, 0, 3)).reshape(N_BAND, slot_count)

    def one_owner(owner):
        source_rows = global_src[owner]
        senders = jnp.take(grid_latent, source_rows, axis=0)
        own_edges = edge_latent[owner].reshape(slot_count, full_width)
        targets = edge_dst[owner].reshape(slot_count)
        mesh_rows = lax.dynamic_slice_in_dim(mesh_latent, (owner * M_DEV).astype(jnp.int32), M_DEV, 0)
        receivers = jnp.take(mesh_rows, jnp.clip(targets, 0, M_DEV - 1), axis=0)
        joined = jnp.concatenate([own_edges, senders, receivers], 1)
        hidden = jnp.dot(joined, edge_w1, preferred_element_type=jnp.float32) + edge_b1
        active = jax.nn.silu(hidden).astype(jnp.bfloat16)
        update = jnp.dot(active, edge_w2, preferred_element_type=jnp.float32) + edge_b2
        edge_new = (own_edges.astype(jnp.float32) + normalize(update, edge_gain, edge_shift)).astype(jnp.bfloat16)
        summed = jax.ops.segment_sum(edge_new.astype(jnp.float32), targets, num_segments=M_DEV + 1)[:M_DEV]
        node_in = jnp.concatenate([mesh_rows, summed.astype(jnp.bfloat16)], 1)
        node_hidden = jnp.dot(node_in, node_w1, preferred_element_type=jnp.float32) + node_b1
        node_active = jax.nn.silu(node_hidden).astype(jnp.bfloat16)
        node_update = jnp.dot(node_active, node_w2, preferred_element_type=jnp.float32) + node_b2
        return (mesh_rows.astype(jnp.float32) + normalize(node_update, node_gain, node_shift)).astype(jnp.bfloat16)
    updated = lax.map(one_owner, jnp.arange(N_BAND, dtype=jnp.int32))
    return updated.reshape(N_BAND * M_DEV, full_width)
```

```python
import functools

import jax
import jax.numpy as jnp
from jax import lax
from jax.experimental import pallas as pl
from jax.experimental.pallas import tpu as pltpu
from jax.sharding import PartitionSpec as P

EPSILON = 1e-05
STEP = 128
GROUP = 8
VMEM = pl.BlockSpec(memory_space=pltpu.VMEM)
SMEM = pl.BlockSpec(memory_space=pltpu.SMEM)
ANY = pl.BlockSpec(memory_space=pl.ANY)


def dot(a, b):
    return jnp.dot(a, b, preferred_element_type=jnp.float32)


def silu(v):
    return v / (1.0 + jnp.exp(-v))


def normalize(values, gain, shift):
    average = jnp.mean(values, -1, keepdims=True)
    centered = values - average
    variance = jnp.mean(centered * centered, -1, keepdims=True)
    return centered * lax.rsqrt(variance + EPSILON) * gain + shift


def pick_kernel(ids, table, out, wide, rows):
    wide[...] = table[...].astype(jnp.float32)

    def some_rows(i, carry):
        base = pl.multiple_of(i * STEP, STEP)
        for r in range(STEP):
            rows[pl.ds(r, 1), :] = wide[pl.ds(ids[base + r], 1), :]
        out[pl.ds(base, STEP), :] = rows[...].astype(jnp.bfloat16)
        return carry

    lax.fori_loop(0, out.shape[0] // STEP, some_rows, 0)


def pick_rows(table, ids):
    return pl.pallas_call(
        pick_kernel,
        out_shape=jax.ShapeDtypeStruct((ids.shape[0], table.shape[1]), jnp.bfloat16),
        in_specs=[SMEM, VMEM],
        out_specs=VMEM,
        scratch_shapes=[
            pltpu.VMEM(table.shape, jnp.float32),
            pltpu.VMEM((STEP, table.shape[1]), jnp.float32),
        ],
        name="pick_rows",
    )(ids, table)


def early_kernel(live, edges, dst_col, mesh_rows, w1, b1, nw1, nb1, pre, node_pre):
    width = edges.shape[1]
    nodes = mesh_rows.shape[0]
    tiles = live.shape[0]
    rows = edges.shape[0] // tiles
    node_pre[...] = dot(mesh_rows[...], nw1[:width, :]) + nb1[...]
    projected = dot(mesh_rows[...], w1[2 * width :, :]) + b1[...]
    high = projected.astype(jnp.bfloat16)
    low = (projected - high.astype(jnp.float32)).astype(jnp.bfloat16)
    ids = lax.broadcasted_iota(jnp.int32, (rows, nodes), 1)

    def tile(t, carry):
        @pl.when(live[t] > 0)
        def _():
            at = pl.ds(pl.multiple_of(t * rows, rows), rows)
            pick = (ids == dst_col[at, :]).astype(jnp.float32).astype(jnp.bfloat16)
            pre[at, :] = dot(edges[at, :], w1[:width, :]) + (dot(pick, high) + dot(pick, low))

        return carry

    lax.fori_loop(0, tiles, tile, 0)


def late_kernel(live, arrived, edges, pre, dst_row, ws, w2, b2, gain, shift, out, held, total, sems):
    width = edges.shape[1]
    nodes = out.shape[0]
    tiles = live.shape[0]
    rows = edges.shape[0] // tiles
    blocks = arrived.shape[1]

    def copy(t):
        return pltpu.make_async_copy(arrived.at[pl.ds(t * GROUP, GROUP)], held.at[t], sems.at[t])

    def start(t, carry):
        @pl.when(live[t] > 0)
        def _():
            copy(t).start()

        return carry

    lax.fori_loop(0, tiles, start, 0)
    total[...] = jnp.zeros_like(total)
    ids = lax.broadcasted_iota(jnp.int32, (nodes, rows), 0)

    def tile(t, carry):
        @pl.when(live[t] > 0)
        def _():
            copy(t).wait()
            at = pl.ds(pl.multiple_of(t * rows, rows), rows)
            senders = jnp.concatenate(
                [held[t, :, f].reshape(rows, width // blocks) for f in range(blocks)], 1
            )
            active = silu(pre[at, :] + dot(senders, ws[...])).astype(jnp.bfloat16)
            update = dot(active, w2[...]) + b2[...]
            new = edges[at, :].astype(jnp.float32) + normalize(update, gain[...], shift[...])
            sel = (ids == dst_row[t]).astype(jnp.float32).astype(jnp.bfloat16)
            total[...] += dot(sel, new.astype(jnp.bfloat16))

        return carry

    lax.fori_loop(0, tiles, tile, 0)
    out[...] = total[...].astype(jnp.bfloat16)


def node_kernel(column, own, one, two, three, node_pre, mesh_rows, nw, w2, b2, gain, shift, out, full):
    f32 = jnp.float32
    quarter = out.shape[1]
    summed = own[...].astype(f32) + one[...].astype(f32) + two[...].astype(f32) + three[...].astype(f32)
    hidden = node_pre[...] + dot(summed.astype(jnp.bfloat16), nw[...])
    update = dot(silu(hidden).astype(jnp.bfloat16), w2[...]) + b2[...]
    full[...] = mesh_rows[...].astype(f32) + normalize(update, gain[...], shift[...])
    at = pl.ds(pl.multiple_of(column[0] * quarter, quarter), quarter)
    out[...] = full[:, at].astype(jnp.bfloat16)


def body(
    grid_latent,
    mesh_latent,
    edge_latent,
    edge_src,
    edge_dst,
    edge_w1,
    edge_b1,
    edge_w2,
    edge_b2,
    edge_gain,
    edge_shift,
    node_w1,
    node_b1,
    node_w2,
    node_b2,
    node_gain,
    node_shift,
):
    bands = lax.axis_size("band")
    feats = lax.axis_size("feat")
    quarter = grid_latent.shape[1]
    width = quarter * feats
    nodes = mesh_latent.shape[0]
    row = lambda v: v.reshape(1, -1)

    picked = pick_rows(grid_latent, edge_src.reshape(-1))
    picked = picked.reshape(bands * feats, -1, quarter)
    arrived = lax.all_to_all(picked, ("band", "feat"), 0, 0, tiled=True)
    arrived = arrived.reshape(bands, feats, -1, quarter)

    edges = edge_latent.reshape(-1, width)
    targets = edge_dst.reshape(-1)
    slots = targets.shape[0]
    tiles = bands // GROUP
    live = jnp.any((targets < nodes).reshape(tiles, -1), 1).astype(jnp.int32)
    mesh_rows = lax.all_gather(mesh_latent, "feat", axis=1, tiled=True)

    pre, node_pre = pl.pallas_call(
        early_kernel,
        out_shape=[
            jax.ShapeDtypeStruct((slots, width), jnp.float32),
            jax.ShapeDtypeStruct((nodes, width), jnp.float32),
        ],
        in_specs=[SMEM] + [VMEM] * 7,
        out_specs=[VMEM] * 2,
        cost_estimate=pl.CostEstimate(
            flops=2 * slots * width * width * 2, bytes_accessed=12 << 20, transcendentals=0
        ),
        name="early",
    )(live, edges, targets.reshape(-1, 1), mesh_rows, edge_w1, row(edge_b1), node_w1, row(node_b1))

    partial = pl.pallas_call(
        late_kernel,
        out_shape=jax.ShapeDtypeStruct((nodes, width), jnp.bfloat16),
        in_specs=[SMEM, ANY] + [VMEM] * 8,
        out_specs=VMEM,
        scratch_shapes=[
            pltpu.VMEM((tiles, GROUP) + arrived.shape[1:], jnp.bfloat16),
            pltpu.VMEM((nodes, width), jnp.float32),
            pltpu.SemaphoreType.DMA((tiles,)),
        ],
        cost_estimate=pl.CostEstimate(
            flops=2 * slots * width * width * 2, bytes_accessed=12 << 20, transcendentals=0
        ),
        name="late",
    )(
        live,
        arrived,
        edges,
        pre,
        targets.reshape(tiles, 1, -1),
        edge_w1[width : 2 * width],
        edge_w2,
        row(edge_b2),
        row(edge_gain),
        row(edge_shift),
    )

    others = [
        lax.ppermute(partial, "feat", [(i, (i + k) % feats) for i in range(feats)])
        for k in range(1, feats)
    ]
    column = jnp.full((1,), lax.axis_index("feat"), jnp.int32)
    return pl.pallas_call(
        node_kernel,
        out_shape=jax.ShapeDtypeStruct((nodes, quarter), jnp.bfloat16),
        in_specs=[SMEM] + [VMEM] * 11,
        out_specs=VMEM,
        scratch_shapes=[pltpu.VMEM((nodes, width), jnp.float32)],
        name="node",
    )(
        column,
        partial,
        *others,
        node_pre,
        mesh_rows,
        node_w1[width:],
        node_w2,
        row(node_b2),
        row(node_gain),
        row(node_shift),
    )


def solution(mesh):
    rep = P()
    placed = (
        P("band", "feat"),
        P("band", "feat"),
        P("band", "feat", None, None),
        P("band", None),
        P("band", "feat", None),
    ) + (rep,) * 12
    return jax.shard_map(
        body, mesh=mesh, in_specs=placed, out_specs=P("band", "feat"), check_vma=False
    )
```

```python
import functools

import jax
import jax.numpy as jnp
from jax import lax
from jax.experimental import pallas as pl
from jax.experimental.pallas import tpu as pltpu
from jax.sharding import PartitionSpec as P

EPSILON = 1e-05
STEP = 128
GROUP = 8
VMEM = pl.BlockSpec(memory_space=pltpu.VMEM)
SMEM = pl.BlockSpec(memory_space=pltpu.SMEM)
HBM = pl.BlockSpec(memory_space=pltpu.HBM)


def in_vmem(value):
    return pltpu.with_memory_space_constraint(value, pltpu.VMEM)


def dot(a, b):
    return jnp.dot(a, b, preferred_element_type=jnp.float32)


def in_hbm(value):
    return pltpu.with_memory_space_constraint(value, pltpu.HBM)


def silu(v):
    return v / (1.0 + jnp.exp(-v))


def normalize(values, gain, shift):
    average = jnp.mean(values, -1, keepdims=True)
    centered = values - average
    variance = jnp.mean(centered * centered, -1, keepdims=True)
    return centered * lax.rsqrt(variance + EPSILON) * gain + shift


def pick_kernel(ids, table, out, wide, rows):
    wide[...] = table[...].astype(jnp.float32)

    def some_rows(i, carry):
        base = pl.multiple_of(i * STEP, STEP)
        for r in range(STEP):
            rows[pl.ds(r, 1), :] = wide[pl.ds(ids[base + r], 1), :]
        out[pl.ds(base, STEP), :] = rows[...].astype(jnp.bfloat16)
        return carry

    lax.fori_loop(0, out.shape[0] // STEP, some_rows, 0)


def pick_rows(table, ids):
    return pl.pallas_call(
        pick_kernel,
        out_shape=jax.ShapeDtypeStruct((ids.shape[0], table.shape[1]), jnp.bfloat16),
        in_specs=[SMEM, VMEM],
        out_specs=VMEM,
        scratch_shapes=[
            pltpu.VMEM(table.shape, jnp.float32),
            pltpu.VMEM((STEP, table.shape[1]), jnp.float32),
        ],
        compiler_params=pltpu.CompilerParams(vmem_limit_bytes=8 << 20),
        name="pick_rows",
    )(ids, table)


def early_kernel(live, edges, dst_col, mesh_rows, w1, b1, nw1, nb1, pre, node_pre):
    width = edges.shape[1]
    nodes = mesh_rows.shape[0]
    tiles = live.shape[0]
    rows = edges.shape[0] // tiles
    node_pre[...] = dot(mesh_rows[...], nw1[:width, :]) + nb1[...]
    projected = dot(mesh_rows[...], w1[2 * width :, :]) + b1[...]
    high = projected.astype(jnp.bfloat16)
    low = (projected - high.astype(jnp.float32)).astype(jnp.bfloat16)
    ids = lax.broadcasted_iota(jnp.int32, (rows, nodes), 1)

    def tile(t, carry):
        @pl.when(live[t] > 0)
        def _():
            at = pl.ds(pl.multiple_of(t * rows, rows), rows)
            pick = (ids == dst_col[at, :]).astype(jnp.float32).astype(jnp.bfloat16)
            pre[at, :] = dot(edges[at, :], w1[:width, :]) + (dot(pick, high) + dot(pick, low))

        return carry

    lax.fori_loop(0, tiles, tile, 0)


def late_kernel(
    live, arrived, edges, pre, dst_row, ws, w2, b2, gain, shift,
    out, edge_tiles, pre_tiles, total, sems,
):
    width = ws.shape[0]
    nodes = out.shape[0]
    tiles, rows = edge_tiles.shape[:2]
    blocks = arrived.shape[1]

    def copies(t):
        at = pl.ds(pl.multiple_of(t * rows, rows), rows)
        return (
            pltpu.make_async_copy(pre.at[at], pre_tiles.at[t], sems.at[0, t]),
            pltpu.make_async_copy(edges.at[at], edge_tiles.at[t], sems.at[1, t]),
        )

    def start(t, carry):
        @pl.when(live[t] > 0)
        def _():
            for copy in copies(t):
                copy.start()

        return carry

    lax.fori_loop(0, tiles, start, 0)
    total[...] = jnp.zeros_like(total)
    ids = lax.broadcasted_iota(jnp.int32, (nodes, rows), 0)

    def tile(t, carry):
        @pl.when(live[t] > 0)
        def _():
            group = pl.ds(t * GROUP, GROUP)
            senders = jnp.concatenate(
                [arrived[group, f].reshape(rows, width // blocks) for f in range(blocks)], 1
            )
            product = dot(senders, ws[...])
            for copy in copies(t):
                copy.wait()
            active = silu(pre_tiles[t] + product).astype(jnp.bfloat16)
            update = dot(active, w2[...]) + b2[...]
            new = edge_tiles[t].astype(jnp.float32) + normalize(update, gain[...], shift[...])
            sel = (ids == dst_row[t]).astype(jnp.float32).astype(jnp.bfloat16)
            total[...] += dot(sel, new.astype(jnp.bfloat16))

        return carry

    lax.fori_loop(0, tiles, tile, 0)
    out[...] = total[...].astype(jnp.bfloat16)


def node_kernel(column, own, one, two, three, node_pre, mesh_rows, nw, w2, b2, gain, shift, out, full):
    f32 = jnp.float32
    quarter = out.shape[1]
    summed = own[...].astype(f32) + one[...].astype(f32) + two[...].astype(f32) + three[...].astype(f32)
    hidden = node_pre[...] + dot(summed.astype(jnp.bfloat16), nw[...])
    update = dot(silu(hidden).astype(jnp.bfloat16), w2[...]) + b2[...]
    full[...] = mesh_rows[...].astype(f32) + normalize(update, gain[...], shift[...])
    at = pl.ds(pl.multiple_of(column[0] * quarter, quarter), quarter)
    out[...] = full[:, at].astype(jnp.bfloat16)


def body(
    grid_latent,
    mesh_latent,
    edge_latent,
    edge_src,
    edge_dst,
    edge_w1,
    edge_b1,
    edge_w2,
    edge_b2,
    edge_gain,
    edge_shift,
    node_w1,
    node_b1,
    node_w2,
    node_b2,
    node_gain,
    node_shift,
):
    bands = lax.axis_size("band")
    feats = lax.axis_size("feat")
    quarter = grid_latent.shape[1]
    width = quarter * feats
    nodes = mesh_latent.shape[0]
    row = lambda v: v.reshape(1, -1)

    picked = pick_rows(grid_latent, edge_src.reshape(-1))
    picked = picked.reshape(bands * feats, -1, quarter)
    arrived = lax.all_to_all(picked, ("band", "feat"), 0, 0, tiled=True)
    arrived = arrived.reshape(bands, feats, -1, quarter)

    edges = edge_latent.reshape(-1, width)
    targets = edge_dst.reshape(-1)
    slots = targets.shape[0]
    tiles = bands // GROUP
    live = jnp.any((targets < nodes).reshape(tiles, -1), 1).astype(jnp.int32)
    mesh_rows = lax.all_gather(mesh_latent, "feat", axis=1, tiled=True)

    pre, node_pre = pl.pallas_call(
        early_kernel,
        out_shape=[
            jax.ShapeDtypeStruct((slots, width), jnp.float32),
            jax.ShapeDtypeStruct((nodes, width), jnp.float32),
        ],
        in_specs=[SMEM] + [VMEM] * 7,
        out_specs=[VMEM] * 2,
        cost_estimate=pl.CostEstimate(
            flops=2 * slots * width * width * 2, bytes_accessed=12 << 20, transcendentals=0
        ),
        compiler_params=pltpu.CompilerParams(vmem_limit_bytes=16 << 20),
        name="early",
    )(live, edges, targets.reshape(-1, 1), mesh_rows, edge_w1, row(edge_b1), node_w1, row(node_b1))

    rows = slots // tiles
    partial = pl.pallas_call(
        late_kernel,
        out_shape=pltpu.VMEM((nodes, width), jnp.bfloat16),
        in_specs=[SMEM, VMEM, HBM, HBM] + [VMEM] * 6,
        out_specs=VMEM,
        scratch_shapes=[
            pltpu.VMEM((tiles, rows, width), jnp.bfloat16),
            pltpu.VMEM((tiles, rows, width), jnp.float32),
            pltpu.VMEM((nodes, width), jnp.float32),
            pltpu.SemaphoreType.DMA((2, tiles)),
        ],
        cost_estimate=pl.CostEstimate(
            flops=2 * slots * width * width * 2, bytes_accessed=12 << 20, transcendentals=0
        ),
        compiler_params=pltpu.CompilerParams(vmem_limit_bytes=20 << 20),
        name="late",
    )(
        live,
        in_vmem(arrived),
        in_hbm(edges),
        in_hbm(pre),
        targets.reshape(tiles, 1, -1),
        in_vmem(edge_w1[width : 2 * width]),
        in_vmem(edge_w2),
        row(edge_b2),
        row(edge_gain),
        row(edge_shift),
    )

    others = [
        lax.ppermute(partial, "feat", [(i, (i + k) % feats) for i in range(feats)])
        for k in range(1, feats)
    ]
    column = jnp.full((1,), lax.axis_index("feat"), jnp.int32)
    return pl.pallas_call(
        node_kernel,
        out_shape=jax.ShapeDtypeStruct((nodes, quarter), jnp.bfloat16),
        in_specs=[SMEM] + [VMEM] * 11,
        out_specs=VMEM,
        scratch_shapes=[pltpu.VMEM((nodes, width), jnp.float32)],
        compiler_params=pltpu.CompilerParams(vmem_limit_bytes=8 << 20),
        name="node",
    )(
        column,
        partial,
        *others,
        node_pre,
        mesh_rows,
        node_w1[width:],
        node_w2,
        row(node_b2),
        row(node_gain),
        row(node_shift),
    )


def solution(mesh):
    rep = P()
    placed = (
        P("band", "feat"),
        P("band", "feat"),
        P("band", "feat", None, None),
        P("band", None),
        P("band", "feat", None),
    ) + (rep,) * 12
    return jax.shard_map(
        body, mesh=mesh, in_specs=placed, out_specs=P("band", "feat"), check_vma=False
    )
```

```python
import functools

import jax
import jax.numpy as jnp
from jax import lax
from jax.experimental import pallas as pl
from jax.experimental.pallas import tpu as pltpu
from jax.sharding import PartitionSpec as P

EPSILON = 1e-05
STEP = 1024
GROUP = 8
VMEM = pl.BlockSpec(memory_space=pltpu.VMEM)
SMEM = pl.BlockSpec(memory_space=pltpu.SMEM)
HBM = pl.BlockSpec(memory_space=pltpu.HBM)


def in_vmem(value):
    return pltpu.with_memory_space_constraint(value, pltpu.VMEM)


def dot(a, b):
    return jnp.dot(a, b, preferred_element_type=jnp.float32)


def in_hbm(value):
    return pltpu.with_memory_space_constraint(value, pltpu.HBM)


def silu(v):
    return v / (1.0 + jnp.exp(-v))


def normalize(values, gain, shift):
    average = jnp.mean(values, -1, keepdims=True)
    centered = values - average
    variance = jnp.mean(centered * centered, -1, keepdims=True)
    return centered * lax.rsqrt(variance + EPSILON) * gain + shift


def pick_kernel(ids, ids_row, table, out, wide, pairs, rows):
    half = table.shape[0] // 2
    by_product = STEP - rows.shape[0]
    pieces = by_product // 128
    per = rows.shape[0] // (pieces * (half // 256))
    wide[...] = table[...].astype(jnp.float32)
    pairs[...] = jnp.concatenate([table[:half], table[half:]], 1)
    lane = lax.broadcasted_iota(jnp.int32, (128, 128), 1)

    def some_rows(i, carry):
        base = pl.multiple_of(i * STEP, STEP)
        r = 0
        for g in range(pieces):
            want = jnp.broadcast_to(ids_row[i * (STEP // 128) + g], (128, 128)).T
            upper = want >= half
            place = jnp.where(upper, want - half, want)
            both = None
            for j in range(half // 256):
                onehot = jnp.concatenate(
                    [
                        jnp.where(place == lane + (256 * j + 128 * u), 1.0, 0.0).astype(jnp.bfloat16)
                        for u in range(2)
                    ],
                    1,
                )
                part = dot(onehot, pairs[256 * j : 256 * (j + 1), :])
                both = part if both is None else both + part
                for _ in range(per):
                    rows[pl.ds(r, 1), :] = wide[pl.ds(ids[base + by_product + r], 1), :]
                    r += 1
            at = pl.ds(pl.multiple_of(base + g * 128, 128), 128)
            out[at, :] = jnp.where(upper, both[:, 128:], both[:, :128]).astype(jnp.bfloat16)
        at = pl.ds(pl.multiple_of(base + by_product, 128), STEP - by_product)
        out[at, :] = rows[...].astype(jnp.bfloat16)
        return carry

    lax.fori_loop(0, out.shape[0] // STEP, some_rows, 0)


def pick_rows(table, ids):
    height, width = table.shape
    return pl.pallas_call(
        pick_kernel,
        out_shape=jax.ShapeDtypeStruct((ids.shape[0], width), jnp.bfloat16),
        in_specs=[SMEM, VMEM, VMEM],
        out_specs=VMEM,
        scratch_shapes=[
            pltpu.VMEM((height, width), jnp.float32),
            pltpu.VMEM((height // 2, 2 * width), jnp.bfloat16),
            pltpu.VMEM((STEP // 2, width), jnp.float32),
        ],
        name="pick_rows",
    )(ids, ids.reshape(-1, 1, 128), table)


def early_kernel(live, edges, dst_col, mesh_rows, w1, b1, nw1, nb1, pre, node_pre):
    width = edges.shape[1]
    nodes = mesh_rows.shape[0]
    tiles = live.shape[0]
    rows = edges.shape[0] // tiles
    node_pre[...] = dot(mesh_rows[...], nw1[:width, :]) + nb1[...]
    projected = dot(mesh_rows[...], w1[2 * width :, :]) + b1[...]
    high = projected.astype(jnp.bfloat16)
    low = (projected - high.astype(jnp.float32)).astype(jnp.bfloat16)
    ids = lax.broadcasted_iota(jnp.int32, (rows, nodes), 1)

    def tile(t, carry):
        @pl.when(live[t] > 0)
        def _():
            at = pl.ds(pl.multiple_of(t * rows, rows), rows)
            pick = (ids == dst_col[at, :]).astype(jnp.float32).astype(jnp.bfloat16)
            pre[at, :] = dot(edges[at, :], w1[:width, :]) + (dot(pick, high) + dot(pick, low))

        return carry

    lax.fori_loop(0, tiles, tile, 0)


def late_kernel(
    live, arrived, edges, pre, dst_row, ws, w2, b2, gain, shift,
    first, second, edge_tiles, pre_tiles, total, sems,
):
    width = ws.shape[0]
    nodes = total.shape[0]
    tiles, rows = edge_tiles.shape[:2]
    blocks = arrived.shape[1]

    def copies(t):
        at = pl.ds(pl.multiple_of(t * rows, rows), rows)
        return (
            pltpu.make_async_copy(pre.at[at], pre_tiles.at[t], sems.at[0, t]),
            pltpu.make_async_copy(edges.at[at], edge_tiles.at[t], sems.at[1, t]),
        )

    def start(t, carry):
        @pl.when(live[t] > 0)
        def _():
            for copy in copies(t):
                copy.start()

        return carry

    lax.fori_loop(0, tiles, start, 0)
    total[...] = jnp.zeros_like(total)
    ids = lax.broadcasted_iota(jnp.int32, (nodes, rows), 0)

    def tile(t, carry):
        @pl.when(live[t] > 0)
        def _():
            group = pl.ds(t * GROUP, GROUP)
            senders = jnp.concatenate(
                [arrived[group, f].reshape(rows, width // blocks) for f in range(blocks)], 1
            )
            product = dot(senders, ws[...])
            for copy in copies(t):
                copy.wait()
            active = silu(pre_tiles[t] + product).astype(jnp.bfloat16)
            update = dot(active, w2[...]) + b2[...]
            new = edge_tiles[t].astype(jnp.float32) + normalize(update, gain[...], shift[...])
            sel = (ids == dst_row[t]).astype(jnp.float32).astype(jnp.bfloat16)
            total[...] += dot(sel, new.astype(jnp.bfloat16))

        return carry

    lax.fori_loop(0, tiles, tile, 0)
    first[...] = total[: nodes // 2, :].astype(jnp.bfloat16)
    second[...] = total[nodes // 2 :, :].astype(jnp.bfloat16)


def node_kernel(
    column, first, first_got, second, second_got, node_pre, mesh_rows, nw, w2, b2, gain, shift,
    out, full, pre_here, w2_here, sems,
):
    f32 = jnp.float32
    quarter = out.shape[1]
    copies = [
        pltpu.make_async_copy(node_pre, pre_here, sems.at[0]),
        pltpu.make_async_copy(w2, w2_here, sems.at[1]),
    ]
    for copy in copies:
        copy.start()
    summed = jnp.concatenate(
        [
            (u[...].astype(f32) + v[...].astype(f32)).astype(jnp.bfloat16)
            for u, v in ((first, first_got), (second, second_got))
        ],
        0,
    )
    hidden = dot(summed, nw[...])
    copies[0].wait()
    active = silu(pre_here[...] + hidden).astype(jnp.bfloat16)
    copies[1].wait()
    update = dot(active, w2_here[...]) + b2[...]
    full[...] = mesh_rows[...].astype(f32) + normalize(update, gain[...], shift[...])
    at = pl.ds(pl.multiple_of(column[0] * quarter, quarter), quarter)
    out[...] = full[:, at].astype(jnp.bfloat16)


def body(
    grid_latent,
    mesh_latent,
    edge_latent,
    edge_src,
    edge_dst,
    edge_w1,
    edge_b1,
    edge_w2,
    edge_b2,
    edge_gain,
    edge_shift,
    node_w1,
    node_b1,
    node_w2,
    node_b2,
    node_gain,
    node_shift,
):
    bands = lax.axis_size("band")
    feats = lax.axis_size("feat")
    quarter = grid_latent.shape[1]
    width = quarter * feats
    nodes = mesh_latent.shape[0]
    row = lambda v: v.reshape(1, -1)

    picked = pick_rows(grid_latent, edge_src.reshape(-1))
    picked = picked.reshape(bands * feats, -1, quarter)
    arrived = lax.all_to_all(picked, ("band", "feat"), 0, 0, tiled=True)
    arrived = arrived.reshape(bands, feats, -1, quarter)

    edges = edge_latent.reshape(-1, width)
    targets = edge_dst.reshape(-1)
    slots = targets.shape[0]
    tiles = bands // GROUP
    live = jnp.any((targets < nodes).reshape(tiles, -1), 1).astype(jnp.int32)
    mesh_rows = lax.all_gather(mesh_latent, "feat", axis=1, tiled=True)

    pre, node_pre = pl.pallas_call(
        early_kernel,
        out_shape=[
            jax.ShapeDtypeStruct((slots, width), jnp.float32),
            jax.ShapeDtypeStruct((nodes, width), jnp.float32),
        ],
        in_specs=[SMEM] + [VMEM] * 7,
        out_specs=[VMEM] * 2,
        cost_estimate=pl.CostEstimate(
            flops=2 * slots * width * width * 2, bytes_accessed=12 << 20, transcendentals=0
        ),
        compiler_params=pltpu.CompilerParams(vmem_limit_bytes=16 << 20),
        name="early",
    )(live, edges, targets.reshape(-1, 1), mesh_rows, edge_w1, row(edge_b1), node_w1, row(node_b1))

    rows = slots // tiles
    first, second = pl.pallas_call(
        late_kernel,
        out_shape=[pltpu.VMEM((nodes // 2, width), jnp.bfloat16)] * 2,
        in_specs=[SMEM, VMEM, HBM, HBM] + [VMEM] * 6,
        out_specs=[VMEM] * 2,
        scratch_shapes=[
            pltpu.VMEM((tiles, rows, width), jnp.bfloat16),
            pltpu.VMEM((tiles, rows, width), jnp.float32),
            pltpu.VMEM((nodes, width), jnp.float32),
            pltpu.SemaphoreType.DMA((2, tiles)),
        ],
        cost_estimate=pl.CostEstimate(
            flops=2 * slots * width * width * 2, bytes_accessed=12 << 20, transcendentals=0
        ),
        compiler_params=pltpu.CompilerParams(vmem_limit_bytes=20 << 20),
        name="late",
    )(
        live,
        in_vmem(arrived),
        in_hbm(edges),
        in_hbm(pre),
        targets.reshape(tiles, 1, -1),
        in_vmem(edge_w1[width : 2 * width]),
        in_vmem(edge_w2),
        row(edge_b2),
        row(edge_gain),
        row(edge_shift),
    )

    pairing = [(i, i ^ 1) for i in range(feats)]
    crossing = [(i, feats - 1 - i) for i in range(feats)]
    first_got = lax.ppermute(first, "feat", pairing)
    second_got = lax.ppermute(second, "feat", crossing)
    add = lambda u, v: (u.astype(jnp.float32) + v.astype(jnp.float32)).astype(jnp.bfloat16)
    first = add(first, first_got)
    second = add(second, second_got)
    first_got = lax.ppermute(first, "feat", crossing)
    second_got = lax.ppermute(second, "feat", pairing)
    column = jnp.full((1,), lax.axis_index("feat"), jnp.int32)
    return pl.pallas_call(
        node_kernel,
        out_shape=jax.ShapeDtypeStruct((nodes, quarter), jnp.bfloat16),
        in_specs=[SMEM] + [VMEM] * 4 + [HBM] + [VMEM] * 2 + [HBM] + [VMEM] * 3,
        out_specs=VMEM,
        scratch_shapes=[
            pltpu.VMEM((nodes, width), jnp.float32),
            pltpu.VMEM((nodes, width), jnp.float32),
            pltpu.VMEM((width, width), jnp.bfloat16),
            pltpu.SemaphoreType.DMA((2,)),
        ],
        compiler_params=pltpu.CompilerParams(vmem_limit_bytes=8 << 20),
        name="node",
    )(
        column,
        first,
        first_got,
        second,
        second_got,
        in_hbm(node_pre),
        mesh_rows,
        node_w1[width:],
        in_hbm(node_w2),
        row(node_b2),
        row(node_gain),
        row(node_shift),
    )


def solution(mesh):
    rep = P()
    placed = (
        P("band", "feat"),
        P("band", "feat"),
        P("band", "feat", None, None),
        P("band", None),
        P("band", "feat", None),
    ) + (rep,) * 12
    return jax.shard_map(
        body, mesh=mesh, in_specs=placed, out_specs=P("band", "feat"), check_vma=False
    )
```

```python
import math

import jax
import jax.numpy as jnp
from jax import lax
from jax.experimental import pallas as pl
from jax.experimental.pallas import tpu as pltpu
from jax.sharding import PartitionSpec as P

EPSILON = 1e-05
SIZES = {"y": 4, "z": 8, "core": 2}
FEATS = 4
SLOTS = 32
BAND = tuple(SIZES)
GROUP = 8
VMEM = pl.BlockSpec(memory_space=pltpu.VMEM)
SMEM = pl.BlockSpec(memory_space=pltpu.SMEM)
HBM = pl.BlockSpec(memory_space=pltpu.HBM)
ANY = pl.BlockSpec(memory_space=pl.ANY)
AUTO = jax.sharding.AxisType.Auto


def in_vmem(value):
    return pltpu.with_memory_space_constraint(value, pltpu.VMEM)


def dot(a, b):
    return jnp.dot(a, b, preferred_element_type=jnp.float32)


def in_hbm(value):
    return pltpu.with_memory_space_constraint(value, pltpu.HBM)


def silu(v):
    return v / (1.0 + jnp.exp(-v))


def normalize(values, gain, shift):
    average = jnp.mean(values, -1, keepdims=True)
    centered = values - average
    variance = jnp.mean(centered * centered, -1, keepdims=True)
    return centered * lax.rsqrt(variance + EPSILON) * gain + shift


def pick_kernel(ids, ids_row, table, out, wide, pairs, rows, held, sems):
    half = table.shape[0] // 2
    count = FEATS * SLOTS
    sends = SIZES["y"] * SIZES["core"]
    step = sends * count
    pieces = sends // 2
    per = (step - pieces * count) // (pieces * (half // 256))
    wide[...] = table[...].astype(jnp.float32)
    pairs[...] = jnp.concatenate([table[:half], table[half:]], 1)
    lane = lax.broadcasted_iota(jnp.int32, (count, 128), 1)

    def copy(z):
        at = pl.ds(pl.multiple_of(z * step, step), step)
        return pltpu.make_async_copy(held.at[at], out.at[at], sems.at[z])

    def band_of(n, z):
        y, core = divmod(n, SIZES["core"])
        return (y * SIZES["z"] + z) * SIZES["core"] + core

    def put(n, z, value):
        y, core = divmod(n, SIZES["core"])
        for f in range(FEATS):
            place = ((core * FEATS + f) * SIZES["y"] + y) * SLOTS
            held[pl.ds(pl.multiple_of(z * step + place, SLOTS), SLOTS), :] = value[f * SLOTS : (f + 1) * SLOTS]

    def one_z(z, carry):
        r = 0
        for g in range(pieces):
            want = jnp.broadcast_to(ids_row[band_of(g, z)], (128, 128)).T
            upper = want >= half
            place = jnp.where(upper, want - half, want)
            both = None
            for j in range(half // 256):
                onehot = jnp.concatenate(
                    [
                        jnp.where(place == lane + (256 * j + 128 * u), 1.0, 0.0).astype(jnp.bfloat16)
                        for u in range(2)
                    ],
                    1,
                )
                part = dot(onehot, pairs[256 * j : 256 * (j + 1), :])
                both = part if both is None else both + part
                for _ in range(per):
                    n, slot = divmod(r, count)
                    rows[pl.ds(r, 1), :] = wide[pl.ds(ids[band_of(pieces + n, z) * count + slot], 1), :]
                    r += 1
            put(g, z, jnp.where(upper, both[:, 128:], both[:, :128]).astype(jnp.bfloat16))
        for n in range(pieces):
            put(pieces + n, z, rows[n * count : (n + 1) * count, :].astype(jnp.bfloat16))
        copy(z).start()
        return carry

    lax.fori_loop(0, SIZES["z"], one_z, 0)

    def finish(z, carry):
        copy(z).wait()
        return carry

    lax.fori_loop(0, SIZES["z"], finish, 0)


def pick_rows(table, ids):
    height, width = table.shape
    per_turn = SIZES["y"] * SIZES["core"] * FEATS * SLOTS
    return pl.pallas_call(
        pick_kernel,
        out_shape=jax.ShapeDtypeStruct((ids.shape[0], width), jnp.bfloat16),
        in_specs=[SMEM, VMEM, VMEM],
        out_specs=ANY,
        scratch_shapes=[
            pltpu.VMEM((height, width), jnp.float32),
            pltpu.VMEM((height // 2, 2 * width), jnp.bfloat16),
            pltpu.VMEM((per_turn // 2, width), jnp.float32),
            pltpu.VMEM((ids.shape[0], width), jnp.bfloat16),
            pltpu.SemaphoreType.DMA((SIZES["z"],)),
        ],
        name="pick_rows",
    )(ids, ids.reshape(-1, 1, 128), table)


def early_kernel(live, edges, dst_col, mesh_rows, w1, b1, nw1, nb1, pre, node_pre):
    width = edges.shape[1]
    nodes = mesh_rows.shape[0]
    tiles = live.shape[0]
    rows = edges.shape[0] // tiles
    node_pre[...] = dot(mesh_rows[...], nw1[:width, :]) + nb1[...]
    projected = dot(mesh_rows[...], w1[2 * width :, :]) + b1[...]
    high = projected.astype(jnp.bfloat16)
    low = (projected - high.astype(jnp.float32)).astype(jnp.bfloat16)
    ids = lax.broadcasted_iota(jnp.int32, (rows, nodes), 1)

    def tile(t, carry):
        @pl.when(live[t] > 0)
        def _():
            at = pl.ds(pl.multiple_of(t * rows, rows), rows)
            pick = (ids == dst_col[at, :]).astype(jnp.float32).astype(jnp.bfloat16)
            pre[at, :] = dot(edges[at, :], w1[:width, :]) + (dot(pick, high) + dot(pick, low))

        return carry

    lax.fori_loop(0, tiles, tile, 0)


def late_kernel(
    live, arrived, edges, pre, dst_row, ws, w2, b2, gain, shift,
    first, second, edge_tiles, pre_tiles, total, sems,
):
    width = ws.shape[0]
    nodes = total.shape[0]
    tiles, rows = edge_tiles.shape[:2]
    cores = SIZES["core"]
    span = GROUP // cores

    def copies(t):
        at = pl.ds(pl.multiple_of(t * rows, rows), rows)
        return (
            pltpu.make_async_copy(pre.at[at], pre_tiles.at[t], sems.at[0, t]),
            pltpu.make_async_copy(edges.at[at], edge_tiles.at[t], sems.at[1, t]),
        )

    def start(t, carry):
        @pl.when(live[t] > 0)
        def _():
            for copy in copies(t):
                copy.start()

        return carry

    lax.fori_loop(0, tiles, start, 0)
    total[...] = jnp.zeros_like(total)
    ids = lax.broadcasted_iota(jnp.int32, (nodes, rows), 0)

    def tile(t, carry):
        @pl.when(live[t] > 0)
        def _():
            turns = SIZES["z"] // span
            y, z = t // turns, lax.rem(t, turns) * span
            senders = jnp.concatenate(
                [
                    jnp.concatenate(
                        [
                            arrived[(((z + n // cores) * cores + n % cores) * FEATS + f) * SIZES["y"] + y]
                            for n in range(GROUP)
                        ],
                        0,
                    )
                    for f in range(FEATS)
                ],
                1,
            )
            product = dot(senders, ws[...])
            for copy in copies(t):
                copy.wait()
            active = silu(pre_tiles[t] + product).astype(jnp.bfloat16)
            update = dot(active, w2[...]) + b2[...]
            new = edge_tiles[t].astype(jnp.float32) + normalize(update, gain[...], shift[...])
            sel = (ids == dst_row[t]).astype(jnp.float32).astype(jnp.bfloat16)
            total[...] += dot(sel, new.astype(jnp.bfloat16))

        return carry

    lax.fori_loop(0, tiles, tile, 0)
    first[...] = total[: nodes // 2, :].astype(jnp.bfloat16)
    second[...] = total[nodes // 2 :, :].astype(jnp.bfloat16)


def node_kernel(
    column, first, first_got, second, second_got, node_pre, mesh_rows, nw, w2, b2, gain, shift,
    out, full, pre_here, w2_here, sems,
):
    f32 = jnp.float32
    quarter = out.shape[1]
    copies = [
        pltpu.make_async_copy(node_pre, pre_here, sems.at[0]),
        pltpu.make_async_copy(w2, w2_here, sems.at[1]),
    ]
    for copy in copies:
        copy.start()
    summed = jnp.concatenate(
        [
            (u[...].astype(f32) + v[...].astype(f32)).astype(jnp.bfloat16)
            for u, v in ((first, first_got), (second, second_got))
        ],
        0,
    )
    hidden = dot(summed, nw[...])
    copies[0].wait()
    active = silu(pre_here[...] + hidden).astype(jnp.bfloat16)
    copies[1].wait()
    update = dot(active, w2_here[...]) + b2[...]
    full[...] = mesh_rows[...].astype(f32) + normalize(update, gain[...], shift[...])
    at = pl.ds(pl.multiple_of(column[0] * quarter, quarter), quarter)
    out[...] = full[:, at].astype(jnp.bfloat16)


def body(
    grid_latent,
    mesh_latent,
    edge_latent,
    edge_src,
    edge_dst,
    edge_w1,
    edge_b1,
    edge_w2,
    edge_b2,
    edge_gain,
    edge_shift,
    node_w1,
    node_b1,
    node_w2,
    node_b2,
    node_gain,
    node_shift,
):
    bands = math.prod(SIZES.values())
    feats = FEATS
    quarter = grid_latent.shape[1]
    width = quarter * feats
    nodes = mesh_latent.shape[0]
    row = lambda v: v.reshape(1, -1)

    picked = pick_rows(grid_latent, edge_src.reshape(-1))
    picked = picked.reshape(bands * feats, -1, quarter)
    arrived = lax.all_to_all(picked, ("z", "core", "feat", "y"), 0, 0, tiled=True)

    edges = edge_latent.reshape(-1, width)
    targets = edge_dst.reshape(-1)
    slots = targets.shape[0]
    tiles = bands // GROUP
    live = jnp.any((targets < nodes).reshape(tiles, -1), 1).astype(jnp.int32)
    mesh_rows = lax.all_gather(mesh_latent, "feat", axis=1, tiled=True)

    pre, node_pre = pl.pallas_call(
        early_kernel,
        out_shape=[
            jax.ShapeDtypeStruct((slots, width), jnp.float32),
            jax.ShapeDtypeStruct((nodes, width), jnp.float32),
        ],
        in_specs=[SMEM] + [VMEM] * 7,
        out_specs=[VMEM] * 2,
        cost_estimate=pl.CostEstimate(
            flops=2 * slots * width * width * 2, bytes_accessed=12 << 20, transcendentals=0
        ),
        compiler_params=pltpu.CompilerParams(vmem_limit_bytes=16 << 20),
        name="early",
    )(live, edges, targets.reshape(-1, 1), mesh_rows, edge_w1, row(edge_b1), node_w1, row(node_b1))

    rows = slots // tiles
    first, second = pl.pallas_call(
        late_kernel,
        out_shape=[pltpu.VMEM((nodes // 2, width), jnp.bfloat16)] * 2,
        in_specs=[SMEM, VMEM, HBM, HBM] + [VMEM] * 6,
        out_specs=[VMEM] * 2,
        scratch_shapes=[
            pltpu.VMEM((tiles, rows, width), jnp.bfloat16),
            pltpu.VMEM((tiles, rows, width), jnp.float32),
            pltpu.VMEM((nodes, width), jnp.float32),
            pltpu.SemaphoreType.DMA((2, tiles)),
        ],
        cost_estimate=pl.CostEstimate(
            flops=2 * slots * width * width * 2, bytes_accessed=12 << 20, transcendentals=0
        ),
        compiler_params=pltpu.CompilerParams(vmem_limit_bytes=20 << 20),
        name="late",
    )(
        live,
        in_vmem(arrived),
        in_hbm(edges),
        in_hbm(pre),
        targets.reshape(tiles, 1, -1),
        in_vmem(edge_w1[width : 2 * width]),
        in_vmem(edge_w2),
        row(edge_b2),
        row(edge_gain),
        row(edge_shift),
    )

    pairing = [(i, i ^ 1) for i in range(feats)]
    crossing = [(i, feats - 1 - i) for i in range(feats)]
    first_got = lax.ppermute(first, "feat", pairing)
    second_got = lax.ppermute(second, "feat", crossing)
    add = lambda u, v: (u.astype(jnp.float32) + v.astype(jnp.float32)).astype(jnp.bfloat16)
    first = add(first, first_got)
    second = add(second, second_got)
    first_got = lax.ppermute(first, "feat", crossing)
    second_got = lax.ppermute(second, "feat", pairing)
    column = jnp.full((1,), lax.axis_index("feat"), jnp.int32)
    return pl.pallas_call(
        node_kernel,
        out_shape=jax.ShapeDtypeStruct((nodes, quarter), jnp.bfloat16),
        in_specs=[SMEM] + [VMEM] * 4 + [HBM] + [VMEM] * 2 + [HBM] + [VMEM] * 3,
        out_specs=VMEM,
        scratch_shapes=[
            pltpu.VMEM((nodes, width), jnp.float32),
            pltpu.VMEM((nodes, width), jnp.float32),
            pltpu.VMEM((width, width), jnp.bfloat16),
            pltpu.SemaphoreType.DMA((2,)),
        ],
        compiler_params=pltpu.CompilerParams(vmem_limit_bytes=8 << 20),
        name="node",
    )(
        column,
        first,
        first_got,
        second,
        second_got,
        in_hbm(node_pre),
        mesh_rows,
        node_w1[width:],
        in_hbm(node_w2),
        row(node_b2),
        row(node_gain),
        row(node_shift),
    )


def solution(mesh):
    parts = jax.sharding.Mesh(
        mesh.devices.reshape(*SIZES.values(), FEATS), BAND + ("feat",), axis_types=(AUTO,) * 4
    )
    placed = (
        P(BAND, "feat"),
        P(BAND, "feat"),
        P(BAND, "feat", None, None),
        P(BAND, None),
        P(BAND, "feat", None),
    ) + (P(),) * 12
    return jax.shard_map(
        body, mesh=parts, in_specs=placed, out_specs=P(BAND, "feat"), check_vma=False
    )
```

```python
import math

import jax
import jax.numpy as jnp
from jax import lax
from jax.experimental import pallas as pl
from jax.experimental.pallas import tpu as pltpu
from jax.sharding import PartitionSpec as P

EPSILON = 1e-05
SIZES = {"y": 4, "z": 8, "core": 2}
FEATS = 4
SLOTS = 32
BAND = tuple(SIZES)
GROUP = 8
VMEM = pl.BlockSpec(memory_space=pltpu.VMEM)
SMEM = pl.BlockSpec(memory_space=pltpu.SMEM)
HBM = pl.BlockSpec(memory_space=pltpu.HBM)
ANY = pl.BlockSpec(memory_space=pl.ANY)
AUTO = jax.sharding.AxisType.Auto


def in_vmem(value):
    return pltpu.with_memory_space_constraint(value, pltpu.VMEM)


def dot(a, b):
    return jnp.dot(a, b, preferred_element_type=jnp.float32)


def in_hbm(value):
    return pltpu.with_memory_space_constraint(value, pltpu.HBM)


def silu(v):
    return v / (1.0 + jnp.exp(-v))


def normalize(values, gain, shift):
    average = jnp.mean(values, -1, keepdims=True)
    centered = values - average
    variance = jnp.mean(centered * centered, -1, keepdims=True)
    return centered * lax.rsqrt(variance + EPSILON) * gain + shift


def pick_kernel(ids, ids_row, table, out, wide, pairs, rows, held, sems):
    half = table.shape[0] // 2
    count = FEATS * SLOTS
    sends = SIZES["y"] * SIZES["core"]
    step = sends * count
    pieces = sends // 2
    per = (step - pieces * count) // (pieces * (half // 256))
    wide[...] = table[...].astype(jnp.float32)
    pairs[...] = jnp.concatenate([table[:half], table[half:]], 1)
    lane = lax.broadcasted_iota(jnp.int32, (count, 128), 1)

    def copy(z):
        at = pl.ds(pl.multiple_of(z * step, step), step)
        return pltpu.make_async_copy(held.at[at], out.at[at], sems.at[z])

    def band_of(n):
        y, core = divmod(n, SIZES["core"])
        return y * SIZES["z"] * SIZES["core"] + core

    def put(n, z, value):
        y, core = divmod(n, SIZES["core"])
        for f in range(FEATS):
            place = ((core * FEATS + f) * SIZES["y"] + y) * SLOTS
            held[pl.ds(pl.multiple_of(z * step + place, SLOTS), SLOTS), :] = value[f * SLOTS : (f + 1) * SLOTS]

    def one_z(z, carry):
        r = 0
        first_band = z * SIZES["core"]
        base = first_band * count
        for g in range(pieces):
            want = jnp.broadcast_to(ids_row[first_band + band_of(g)], (128, 128)).T
            upper = want >= half
            place = jnp.where(upper, want - half, want)
            both = None
            for j in range(half // 256):
                onehot = jnp.concatenate(
                    [
                        jnp.where(place == lane + (256 * j + 128 * u), 1.0, 0.0).astype(jnp.bfloat16)
                        for u in range(2)
                    ],
                    1,
                )
                part = dot(onehot, pairs[256 * j : 256 * (j + 1), :])
                both = part if both is None else both + part
                for _ in range(per):
                    n, slot = divmod(r, count)
                    rows[pl.ds(r, 1), :] = wide[pl.ds(ids[base + (band_of(pieces + n) * count + slot)], 1), :]
                    r += 1
            put(g, z, jnp.where(upper, both[:, 128:], both[:, :128]).astype(jnp.bfloat16))
        for n in range(pieces):
            put(pieces + n, z, rows[n * count : (n + 1) * count, :].astype(jnp.bfloat16))
        copy(z).start()
        return carry

    lax.fori_loop(0, SIZES["z"], one_z, 0)

    def finish(z, carry):
        copy(z).wait()
        return carry

    lax.fori_loop(0, SIZES["z"], finish, 0)


def pick_rows(table, ids):
    height, width = table.shape
    per_turn = SIZES["y"] * SIZES["core"] * FEATS * SLOTS
    return pl.pallas_call(
        pick_kernel,
        out_shape=jax.ShapeDtypeStruct((ids.shape[0], width), jnp.bfloat16),
        in_specs=[SMEM, VMEM, VMEM],
        out_specs=ANY,
        scratch_shapes=[
            pltpu.VMEM((height, width), jnp.float32),
            pltpu.VMEM((height // 2, 2 * width), jnp.bfloat16),
            pltpu.VMEM((per_turn // 2, width), jnp.float32),
            pltpu.VMEM((ids.shape[0], width), jnp.bfloat16),
            pltpu.SemaphoreType.DMA((SIZES["z"],)),
        ],
        name="pick_rows",
    )(ids, ids.reshape(-1, 1, 128), table)


def early_kernel(live, edges, dst_col, mesh_rows, w1, b1, nw1, nb1, pre, node_pre):
    width = edges.shape[1]
    nodes = mesh_rows.shape[0]
    tiles = live.shape[0]
    rows = edges.shape[0] // tiles
    node_pre[...] = dot(mesh_rows[...], nw1[:width, :]) + nb1[...]
    projected = dot(mesh_rows[...], w1[2 * width :, :]) + b1[...]
    high = projected.astype(jnp.bfloat16)
    low = (projected - high.astype(jnp.float32)).astype(jnp.bfloat16)
    ids = lax.broadcasted_iota(jnp.int32, (rows, nodes), 1)

    def tile(t, carry):
        @pl.when(live[t] > 0)
        def _():
            at = pl.ds(pl.multiple_of(t * rows, rows), rows)
            pick = (ids == dst_col[at, :]).astype(jnp.float32).astype(jnp.bfloat16)
            pre[at, :] = dot(edges[at, :], w1[:width, :]) + (dot(pick, high) + dot(pick, low))

        return carry

    lax.fori_loop(0, tiles, tile, 0)


def late_kernel(
    live, arrived, edges, pre, dst_row, ws, w2, b2, gain, shift,
    first, second, edge_tiles, pre_tiles, total, sems,
):
    width = ws.shape[0]
    nodes = total.shape[0]
    tiles, rows = edge_tiles.shape[:2]
    cores = SIZES["core"]
    span = GROUP // cores

    def copies(t):
        at = pl.ds(pl.multiple_of(t * rows, rows), rows)
        return (
            pltpu.make_async_copy(pre.at[at], pre_tiles.at[t], sems.at[0, t]),
            pltpu.make_async_copy(edges.at[at], edge_tiles.at[t], sems.at[1, t]),
        )

    def start(t, carry):
        @pl.when(live[t] > 0)
        def _():
            for copy in copies(t):
                copy.start()

        return carry

    lax.fori_loop(0, tiles, start, 0)
    total[...] = jnp.zeros_like(total)
    ids = lax.broadcasted_iota(jnp.int32, (nodes, rows), 0)

    def tile(t, carry):
        @pl.when(live[t] > 0)
        def _():
            turns = SIZES["z"] // span
            y, z = t // turns, lax.rem(t, turns) * span
            senders = jnp.concatenate(
                [
                    jnp.concatenate(
                        [
                            arrived[(((z + n // cores) * cores + n % cores) * FEATS + f) * SIZES["y"] + y]
                            for n in range(GROUP)
                        ],
                        0,
                    )
                    for f in range(FEATS)
                ],
                1,
            )
            product = dot(senders, ws[...])
            for copy in copies(t):
                copy.wait()
            active = silu(pre_tiles[t] + product).astype(jnp.bfloat16)
            update = dot(active, w2[...]) + b2[...]
            new = edge_tiles[t].astype(jnp.float32) + normalize(update, gain[...], shift[...])
            sel = (ids == dst_row[t]).astype(jnp.float32).astype(jnp.bfloat16)
            total[...] += dot(sel, new.astype(jnp.bfloat16))

        return carry

    lax.fori_loop(0, tiles, tile, 0)
    first[...] = total[: nodes // 2, :].astype(jnp.bfloat16)
    second[...] = total[nodes // 2 :, :].astype(jnp.bfloat16)


def node_kernel(
    column, first, first_got, second, second_got, node_pre, mesh_rows, nw, w2, b2, gain, shift,
    out, full, pre_here, w2_here, sems,
):
    f32 = jnp.float32
    quarter = out.shape[1]
    copies = [
        pltpu.make_async_copy(node_pre, pre_here, sems.at[0]),
        pltpu.make_async_copy(w2, w2_here, sems.at[1]),
    ]
    for copy in copies:
        copy.start()
    summed = jnp.concatenate(
        [
            (u[...].astype(f32) + v[...].astype(f32)).astype(jnp.bfloat16)
            for u, v in ((first, first_got), (second, second_got))
        ],
        0,
    )
    hidden = dot(summed, nw[...])
    copies[0].wait()
    active = silu(pre_here[...] + hidden).astype(jnp.bfloat16)
    copies[1].wait()
    update = dot(active, w2_here[...]) + b2[...]
    full[...] = mesh_rows[...].astype(f32) + normalize(update, gain[...], shift[...])
    at = pl.ds(pl.multiple_of(column[0] * quarter, quarter), quarter)
    out[...] = full[:, at].astype(jnp.bfloat16)


def body(
    grid_latent,
    mesh_latent,
    edge_latent,
    edge_src,
    edge_dst,
    edge_w1,
    edge_b1,
    edge_w2,
    edge_b2,
    edge_gain,
    edge_shift,
    node_w1,
    node_b1,
    node_w2,
    node_b2,
    node_gain,
    node_shift,
):
    bands = math.prod(SIZES.values())
    feats = FEATS
    quarter = grid_latent.shape[1]
    width = quarter * feats
    nodes = mesh_latent.shape[0]
    row = lambda v: v.reshape(1, -1)

    picked = pick_rows(grid_latent, edge_src.reshape(-1))
    picked = picked.reshape(bands * feats, -1, quarter)
    arrived = lax.all_to_all(picked, ("z", "core", "feat", "y"), 0, 0, tiled=True)

    edges = edge_latent.reshape(-1, width)
    targets = edge_dst.reshape(-1)
    slots = targets.shape[0]
    tiles = bands // GROUP
    live = jnp.any((targets < nodes).reshape(tiles, -1), 1).astype(jnp.int32)
    mesh_rows = lax.all_gather(mesh_latent, "feat", axis=1, tiled=True)

    pre, node_pre = pl.pallas_call(
        early_kernel,
        out_shape=[
            jax.ShapeDtypeStruct((slots, width), jnp.float32),
            jax.ShapeDtypeStruct((nodes, width), jnp.float32),
        ],
        in_specs=[SMEM] + [VMEM] * 7,
        out_specs=[VMEM] * 2,
        cost_estimate=pl.CostEstimate(
            flops=2 * slots * width * width * 2, bytes_accessed=12 << 20, transcendentals=0
        ),
        compiler_params=pltpu.CompilerParams(vmem_limit_bytes=16 << 20),
        name="early",
    )(live, edges, targets.reshape(-1, 1), mesh_rows, edge_w1, row(edge_b1), node_w1, row(node_b1))

    rows = slots // tiles
    first, second = pl.pallas_call(
        late_kernel,
        out_shape=[pltpu.VMEM((nodes // 2, width), jnp.bfloat16)] * 2,
        in_specs=[SMEM, VMEM, HBM, HBM] + [VMEM] * 6,
        out_specs=[VMEM] * 2,
        scratch_shapes=[
            pltpu.VMEM((tiles, rows, width), jnp.bfloat16),
            pltpu.VMEM((tiles, rows, width), jnp.float32),
            pltpu.VMEM((nodes, width), jnp.float32),
            pltpu.SemaphoreType.DMA((2, tiles)),
        ],
        cost_estimate=pl.CostEstimate(
            flops=2 * slots * width * width * 2, bytes_accessed=12 << 20, transcendentals=0
        ),
        compiler_params=pltpu.CompilerParams(vmem_limit_bytes=20 << 20),
        name="late",
    )(
        live,
        in_vmem(arrived),
        in_hbm(edges),
        in_hbm(pre),
        targets.reshape(tiles, 1, -1),
        in_vmem(edge_w1[width : 2 * width]),
        in_vmem(edge_w2),
        row(edge_b2),
        row(edge_gain),
        row(edge_shift),
    )

    pairing = [(i, i ^ 1) for i in range(feats)]
    crossing = [(i, feats - 1 - i) for i in range(feats)]
    first_got = lax.ppermute(first, "feat", pairing)
    second_got = lax.ppermute(second, "feat", crossing)
    add = lambda u, v: (u.astype(jnp.float32) + v.astype(jnp.float32)).astype(jnp.bfloat16)
    first = add(first, first_got)
    second = add(second, second_got)
    first_got = lax.ppermute(first, "feat", crossing)
    second_got = lax.ppermute(second, "feat", pairing)
    column = jnp.full((1,), lax.axis_index("feat"), jnp.int32)
    return pl.pallas_call(
        node_kernel,
        out_shape=jax.ShapeDtypeStruct((nodes, quarter), jnp.bfloat16),
        in_specs=[SMEM] + [VMEM] * 4 + [HBM] + [VMEM] * 2 + [HBM] + [VMEM] * 3,
        out_specs=VMEM,
        scratch_shapes=[
            pltpu.VMEM((nodes, width), jnp.float32),
            pltpu.VMEM((nodes, width), jnp.float32),
            pltpu.VMEM((width, width), jnp.bfloat16),
            pltpu.SemaphoreType.DMA((2,)),
        ],
        compiler_params=pltpu.CompilerParams(vmem_limit_bytes=8 << 20),
        name="node",
    )(
        column,
        first,
        first_got,
        second,
        second_got,
        in_hbm(node_pre),
        mesh_rows,
        node_w1[width:],
        in_hbm(node_w2),
        row(node_b2),
        row(node_gain),
        row(node_shift),
    )


def solution(mesh):
    parts = jax.sharding.Mesh(
        mesh.devices.reshape(*SIZES.values(), FEATS), BAND + ("feat",), axis_types=(AUTO,) * 4
    )
    placed = (
        P(BAND, "feat"),
        P(BAND, "feat"),
        P(BAND, "feat", None, None),
        P(BAND, None),
        P(BAND, "feat", None),
    ) + (P(),) * 12
    return jax.shard_map(
        body, mesh=parts, in_specs=placed, out_specs=P(BAND, "feat"), check_vma=False
    )
```

```python
import math

import jax
import jax.numpy as jnp
from jax import lax
from jax.experimental import pallas as pl
from jax.experimental.pallas import tpu as pltpu
from jax.sharding import PartitionSpec as P

EPSILON = 1e-05
SIZES = {"y": 4, "z": 8, "core": 2}
FEATS = 4
SLOTS = 32
BAND = tuple(SIZES)
GROUP = 8
VMEM = pl.BlockSpec(memory_space=pltpu.VMEM)
SMEM = pl.BlockSpec(memory_space=pltpu.SMEM)
HBM = pl.BlockSpec(memory_space=pltpu.HBM)
ANY = pl.BlockSpec(memory_space=pl.ANY)
AUTO = jax.sharding.AxisType.Auto


def in_vmem(value):
    return pltpu.with_memory_space_constraint(value, pltpu.VMEM)


def dot(a, b):
    return jnp.dot(a, b, preferred_element_type=jnp.float32)


def in_hbm(value):
    return pltpu.with_memory_space_constraint(value, pltpu.HBM)


def silu(v):
    return v / (1.0 + jnp.exp(-v))


def normalize(values, gain, shift):
    average = jnp.mean(values, -1, keepdims=True)
    centered = values - average
    variance = jnp.mean(centered * centered, -1, keepdims=True)
    return centered * lax.rsqrt(variance + EPSILON) * gain + shift


def pick_kernel(ids, ids_row, table, held, wide, pairs, rows):
    half = table.shape[0] // 2
    count = FEATS * SLOTS
    sends = SIZES["y"] * SIZES["core"]
    step = sends * count
    pieces = sends // 2
    per = (step - pieces * count) // (pieces * (half // 256))
    wide[...] = table[...].astype(jnp.float32)
    pairs[...] = jnp.concatenate([table[:half], table[half:]], 1)
    lane = lax.broadcasted_iota(jnp.int32, (count, 128), 1)

    def band_of(n):
        y, core = divmod(n, SIZES["core"])
        return y * SIZES["z"] * SIZES["core"] + core

    def put(n, z, value):
        y, core = divmod(n, SIZES["core"])
        for f in range(FEATS):
            place = ((core * FEATS + f) * SIZES["y"] + y) * SLOTS
            held[pl.ds(pl.multiple_of(z * step + place, SLOTS), SLOTS), :] = value[f * SLOTS : (f + 1) * SLOTS]

    def one_z(z, carry):
        r = 0
        first_band = z * SIZES["core"]
        base = first_band * count
        for g in range(pieces):
            want = jnp.broadcast_to(ids_row[first_band + band_of(g)], (128, 128)).T
            upper = want >= half
            place = jnp.where(upper, want - half, want)
            both = None
            for j in range(half // 256):
                onehot = jnp.concatenate(
                    [
                        jnp.where(place == lane + (256 * j + 128 * u), 1.0, 0.0).astype(jnp.bfloat16)
                        for u in range(2)
                    ],
                    1,
                )
                part = dot(onehot, pairs[256 * j : 256 * (j + 1), :])
                both = part if both is None else both + part
                for _ in range(per):
                    n, slot = divmod(r, count)
                    rows[pl.ds(r, 1), :] = wide[pl.ds(ids[base + (band_of(pieces + n) * count + slot)], 1), :]
                    r += 1
            put(g, z, jnp.where(upper, both[:, 128:], both[:, :128]).astype(jnp.bfloat16))
        for n in range(pieces):
            put(pieces + n, z, rows[n * count : (n + 1) * count, :].astype(jnp.bfloat16))
        return carry

    lax.fori_loop(0, SIZES["z"], one_z, 0)


def pick_rows(table, ids):
    height, width = table.shape
    per_turn = SIZES["y"] * SIZES["core"] * FEATS * SLOTS
    return pl.pallas_call(
        pick_kernel,
        out_shape=jax.ShapeDtypeStruct((ids.shape[0], width), jnp.bfloat16),
        in_specs=[SMEM, VMEM, VMEM],
        out_specs=VMEM,
        scratch_shapes=[
            pltpu.VMEM((height, width), jnp.float32),
            pltpu.VMEM((height // 2, 2 * width), jnp.bfloat16),
            pltpu.VMEM((per_turn // 2, width), jnp.float32),
        ],
        name="pick_rows",
    )(ids, ids.reshape(-1, 1, 128), table)


def early_kernel(live, edges, dst_col, mesh_rows, w1, b1, nw1, nb1, pre, node_pre):
    width = edges.shape[1]
    nodes = mesh_rows.shape[0]
    tiles = live.shape[0]
    rows = edges.shape[0] // tiles
    node_pre[...] = dot(mesh_rows[...], nw1[:width, :]) + nb1[...]
    projected = dot(mesh_rows[...], w1[2 * width :, :]) + b1[...]
    high = projected.astype(jnp.bfloat16)
    low = (projected - high.astype(jnp.float32)).astype(jnp.bfloat16)
    ids = lax.broadcasted_iota(jnp.int32, (rows, nodes), 1)

    def tile(t, carry):
        @pl.when(live[t] > 0)
        def _():
            at = pl.ds(pl.multiple_of(t * rows, rows), rows)
            pick = (ids == dst_col[at, :]).astype(jnp.float32).astype(jnp.bfloat16)
            pre[at, :] = dot(edges[at, :], w1[:width, :]) + (dot(pick, high) + dot(pick, low))

        return carry

    lax.fori_loop(0, tiles, tile, 0)


def late_kernel(
    live, arrived, edges, pre, dst_row, ws, w2, b2, gain, shift,
    first, second, edge_tiles, pre_tiles, total, sems,
):
    width = ws.shape[0]
    nodes = total.shape[0]
    tiles, rows = edge_tiles.shape[:2]
    cores = SIZES["core"]
    span = GROUP // cores

    def copies(t):
        at = pl.ds(pl.multiple_of(t * rows, rows), rows)
        return (
            pltpu.make_async_copy(pre.at[at], pre_tiles.at[t], sems.at[0, t]),
            pltpu.make_async_copy(edges.at[at], edge_tiles.at[t], sems.at[1, t]),
        )

    def start(t, carry):
        @pl.when(live[t] > 0)
        def _():
            for copy in copies(t):
                copy.start()

        return carry

    lax.fori_loop(0, tiles, start, 0)
    total[...] = jnp.zeros_like(total)
    ids = lax.broadcasted_iota(jnp.int32, (nodes, rows), 0)

    def tile(t, carry):
        @pl.when(live[t] > 0)
        def _():
            turns = SIZES["z"] // span
            y, z = t // turns, lax.rem(t, turns) * span
            senders = jnp.concatenate(
                [
                    jnp.concatenate(
                        [
                            arrived[(((z + n // cores) * cores + n % cores) * FEATS + f) * SIZES["y"] + y]
                            for n in range(GROUP)
                        ],
                        0,
                    )
                    for f in range(FEATS)
                ],
                1,
            )
            product = dot(senders, ws[...])
            for copy in copies(t):
                copy.wait()
            active = silu(pre_tiles[t] + product).astype(jnp.bfloat16)
            update = dot(active, w2[...]) + b2[...]
            new = edge_tiles[t].astype(jnp.float32) + normalize(update, gain[...], shift[...])
            sel = (ids == dst_row[t]).astype(jnp.float32).astype(jnp.bfloat16)
            total[...] += dot(sel, new.astype(jnp.bfloat16))

        return carry

    lax.fori_loop(0, tiles, tile, 0)
    first[...] = total[: nodes // 2, :].astype(jnp.bfloat16)
    second[...] = total[nodes // 2 :, :].astype(jnp.bfloat16)


def node_kernel(
    column, first, first_got, second, second_got, node_pre, mesh_rows, nw, w2, b2, gain, shift,
    out, full, pre_here, w2_here, sems,
):
    f32 = jnp.float32
    quarter = out.shape[1]
    copies = [
        pltpu.make_async_copy(node_pre, pre_here, sems.at[0]),
        pltpu.make_async_copy(w2, w2_here, sems.at[1]),
    ]
    for copy in copies:
        copy.start()
    summed = jnp.concatenate(
        [
            (u[...].astype(f32) + v[...].astype(f32)).astype(jnp.bfloat16)
            for u, v in ((first, first_got), (second, second_got))
        ],
        0,
    )
    hidden = dot(summed, nw[...])
    copies[0].wait()
    active = silu(pre_here[...] + hidden).astype(jnp.bfloat16)
    copies[1].wait()
    update = dot(active, w2_here[...]) + b2[...]
    full[...] = mesh_rows[...].astype(f32) + normalize(update, gain[...], shift[...])
    at = pl.ds(pl.multiple_of(column[0] * quarter, quarter), quarter)
    out[...] = full[:, at].astype(jnp.bfloat16)


def body(
    grid_latent,
    mesh_latent,
    edge_latent,
    edge_src,
    edge_dst,
    edge_w1,
    edge_b1,
    edge_w2,
    edge_b2,
    edge_gain,
    edge_shift,
    node_w1,
    node_b1,
    node_w2,
    node_b2,
    node_gain,
    node_shift,
):
    bands = math.prod(SIZES.values())
    feats = FEATS
    quarter = grid_latent.shape[1]
    width = quarter * feats
    nodes = mesh_latent.shape[0]
    row = lambda v: v.reshape(1, -1)

    picked = pick_rows(grid_latent, edge_src.reshape(-1))
    picked = picked.reshape(bands * feats, -1, quarter)
    arrived = lax.all_to_all(picked, ("z", "core", "feat", "y"), 0, 0, tiled=True)

    edges = edge_latent.reshape(-1, width)
    targets = edge_dst.reshape(-1)
    slots = targets.shape[0]
    tiles = bands // GROUP
    live = jnp.any((targets < nodes).reshape(tiles, -1), 1).astype(jnp.int32)
    mesh_rows = lax.all_gather(mesh_latent, "feat", axis=1, tiled=True)

    pre, node_pre = pl.pallas_call(
        early_kernel,
        out_shape=[
            jax.ShapeDtypeStruct((slots, width), jnp.float32),
            jax.ShapeDtypeStruct((nodes, width), jnp.float32),
        ],
        in_specs=[SMEM] + [VMEM] * 7,
        out_specs=[VMEM] * 2,
        cost_estimate=pl.CostEstimate(
            flops=2 * slots * width * width * 2, bytes_accessed=12 << 20, transcendentals=0
        ),
        compiler_params=pltpu.CompilerParams(vmem_limit_bytes=16 << 20),
        name="early",
    )(live, edges, targets.reshape(-1, 1), mesh_rows, edge_w1, row(edge_b1), node_w1, row(node_b1))

    rows = slots // tiles
    first, second = pl.pallas_call(
        late_kernel,
        out_shape=[pltpu.VMEM((nodes // 2, width), jnp.bfloat16)] * 2,
        in_specs=[SMEM, VMEM, HBM, HBM] + [VMEM] * 6,
        out_specs=[VMEM] * 2,
        scratch_shapes=[
            pltpu.VMEM((tiles, rows, width), jnp.bfloat16),
            pltpu.VMEM((tiles, rows, width), jnp.float32),
            pltpu.VMEM((nodes, width), jnp.float32),
            pltpu.SemaphoreType.DMA((2, tiles)),
        ],
        cost_estimate=pl.CostEstimate(
            flops=2 * slots * width * width * 2, bytes_accessed=12 << 20, transcendentals=0
        ),
        compiler_params=pltpu.CompilerParams(vmem_limit_bytes=20 << 20),
        name="late",
    )(
        live,
        in_vmem(arrived),
        in_hbm(edges),
        in_hbm(pre),
        targets.reshape(tiles, 1, -1),
        in_vmem(edge_w1[width : 2 * width]),
        in_vmem(edge_w2),
        row(edge_b2),
        row(edge_gain),
        row(edge_shift),
    )

    pairing = [(i, i ^ 1) for i in range(feats)]
    crossing = [(i, feats - 1 - i) for i in range(feats)]
    first_got = lax.ppermute(first, "feat", pairing)
    second_got = lax.ppermute(second, "feat", crossing)
    add = lambda u, v: (u.astype(jnp.float32) + v.astype(jnp.float32)).astype(jnp.bfloat16)
    first = add(first, first_got)
    second = add(second, second_got)
    first_got = lax.ppermute(first, "feat", crossing)
    second_got = lax.ppermute(second, "feat", pairing)
    column = jnp.full((1,), lax.axis_index("feat"), jnp.int32)
    return pl.pallas_call(
        node_kernel,
        out_shape=jax.ShapeDtypeStruct((nodes, quarter), jnp.bfloat16),
        in_specs=[SMEM] + [VMEM] * 4 + [HBM] + [VMEM] * 2 + [HBM] + [VMEM] * 3,
        out_specs=VMEM,
        scratch_shapes=[
            pltpu.VMEM((nodes, width), jnp.float32),
            pltpu.VMEM((nodes, width), jnp.float32),
            pltpu.VMEM((width, width), jnp.bfloat16),
            pltpu.SemaphoreType.DMA((2,)),
        ],
        compiler_params=pltpu.CompilerParams(vmem_limit_bytes=8 << 20),
        name="node",
    )(
        column,
        first,
        first_got,
        second,
        second_got,
        in_hbm(node_pre),
        mesh_rows,
        node_w1[width:],
        in_hbm(node_w2),
        row(node_b2),
        row(node_gain),
        row(node_shift),
    )


def solution(mesh):
    parts = jax.sharding.Mesh(
        mesh.devices.reshape(*SIZES.values(), FEATS), BAND + ("feat",), axis_types=(AUTO,) * 4
    )
    placed = (
        P(BAND, "feat"),
        P(BAND, "feat"),
        P(BAND, "feat", None, None),
        P(BAND, None),
        P(BAND, "feat", None),
    ) + (P(),) * 12
    return jax.shard_map(
        body, mesh=parts, in_specs=placed, out_specs=P(BAND, "feat"), check_vma=False
    )
```

```python
import math

import jax
import jax.numpy as jnp
from jax import lax
from jax.experimental import pallas as pl
from jax.experimental.pallas import tpu as pltpu
from jax.sharding import PartitionSpec as P

EPSILON = 1e-05
SIZES = {"y": 4, "z": 8, "core": 2}
FEATS = 4
SLOTS = 32
BAND = tuple(SIZES)
GROUP = 8
VMEM = pl.BlockSpec(memory_space=pltpu.VMEM)
SMEM = pl.BlockSpec(memory_space=pltpu.SMEM)
HBM = pl.BlockSpec(memory_space=pltpu.HBM)
ANY = pl.BlockSpec(memory_space=pl.ANY)
AUTO = jax.sharding.AxisType.Auto


def in_vmem(value):
    return pltpu.with_memory_space_constraint(value, pltpu.VMEM)


def dot(a, b):
    return jnp.dot(a, b, preferred_element_type=jnp.float32)


def in_hbm(value):
    return pltpu.with_memory_space_constraint(value, pltpu.HBM)


def silu(v):
    return v / (1.0 + jnp.exp(-v))


def normalize(values, gain, shift):
    average = jnp.mean(values, -1, keepdims=True)
    centered = values - average
    variance = jnp.mean(centered * centered, -1, keepdims=True)
    return centered * lax.rsqrt(variance + EPSILON) * gain + shift


def pick_kernel(ids, ids_row, table, held, wide, pairs, rows):
    half = table.shape[0] // 2
    count = FEATS * SLOTS
    sends = SIZES["y"] * SIZES["core"]
    step = sends * count
    pieces = sends // 2
    per = (step - pieces * count) // (pieces * (half // 256))
    wide[...] = table[...].astype(jnp.float32)
    pairs[...] = jnp.concatenate([table[:half], table[half:]], 1)
    lane = lax.broadcasted_iota(jnp.int32, (count, 128), 1)

    def band_of(n):
        y, core = divmod(n, SIZES["core"])
        return y * SIZES["z"] * SIZES["core"] + core

    def put(n, z, value):
        y, core = divmod(n, SIZES["core"])
        for f in range(FEATS):
            place = ((core * FEATS + f) * SIZES["y"] + y) * SLOTS
            held[pl.ds(pl.multiple_of(z * step + place, SLOTS), SLOTS), :] = value[f * SLOTS : (f + 1) * SLOTS]

    def one_z(z, carry):
        r = 0
        first_band = z * SIZES["core"]
        base = first_band * count
        for g in range(pieces):
            want = jnp.broadcast_to(ids_row[first_band + band_of(g)], (128, 128)).T
            upper = want >= half
            place = jnp.where(upper, want - half, want)
            both = None
            for j in range(half // 256):
                onehot = jnp.concatenate(
                    [
                        jnp.where(place == lane + (256 * j + 128 * u), 1.0, 0.0).astype(jnp.bfloat16)
                        for u in range(2)
                    ],
                    1,
                )
                part = dot(onehot, pairs[256 * j : 256 * (j + 1), :])
                both = part if both is None else both + part
                for _ in range(per):
                    n, slot = divmod(r, count)
                    rows[pl.ds(r, 1), :] = wide[pl.ds(ids[base + (band_of(pieces + n) * count + slot)], 1), :]
                    r += 1
            put(g, z, jnp.where(upper, both[:, 128:], both[:, :128]).astype(jnp.bfloat16))
        for n in range(pieces):
            put(pieces + n, z, rows[n * count : (n + 1) * count, :].astype(jnp.bfloat16))
        return carry

    lax.fori_loop(0, SIZES["z"], one_z, 0)


def pick_rows(table, ids):
    height, width = table.shape
    per_turn = SIZES["y"] * SIZES["core"] * FEATS * SLOTS
    return pl.pallas_call(
        pick_kernel,
        out_shape=jax.ShapeDtypeStruct((ids.shape[0], width), jnp.bfloat16),
        in_specs=[SMEM, VMEM, VMEM],
        out_specs=VMEM,
        scratch_shapes=[
            pltpu.VMEM((height, width), jnp.float32),
            pltpu.VMEM((height // 2, 2 * width), jnp.bfloat16),
            pltpu.VMEM((per_turn // 2, width), jnp.float32),
        ],
        name="pick_rows",
    )(ids, ids.reshape(-1, 1, 128), table)


def early_kernel(live, edges, dst_col, mesh_rows, w1, b1, nw1, nb1, pre, node_pre):
    width = edges.shape[1]
    nodes = mesh_rows.shape[0]
    tiles = live.shape[0]
    rows = edges.shape[0] // tiles
    node_pre[...] = dot(mesh_rows[...], nw1[:width, :]) + nb1[...]
    projected = dot(mesh_rows[...], w1[2 * width :, :]) + b1[...]
    high = projected.astype(jnp.bfloat16)
    low = (projected - high.astype(jnp.float32)).astype(jnp.bfloat16)
    ids = lax.broadcasted_iota(jnp.int32, (rows, nodes), 1)

    def tile(t, carry):
        @pl.when(live[t] > 0)
        def _():
            at = pl.ds(pl.multiple_of(t * rows, rows), rows)
            pick = (ids == dst_col[at, :]).astype(jnp.float32).astype(jnp.bfloat16)
            pre[at, :] = dot(edges[at, :], w1[:width, :]) + (dot(pick, high) + dot(pick, low))

        return carry

    lax.fori_loop(0, tiles, tile, 0)


def late_kernel(
    live, arrived, edges, pre, dst_row, ws, w2, b2, gain, shift,
    first, second, edge_tiles, pre_tiles, total, sems,
):
    width = ws.shape[0]
    nodes = total.shape[0]
    tiles, rows = edge_tiles.shape[:2]
    cores = SIZES["core"]
    span = GROUP // cores

    def copies(t):
        at = pl.ds(pl.multiple_of(t * rows, rows), rows)
        return (
            pltpu.make_async_copy(pre.at[at], pre_tiles.at[t], sems.at[0, t]),
            pltpu.make_async_copy(edges.at[at], edge_tiles.at[t], sems.at[1, t]),
        )

    def start(t, carry):
        @pl.when(live[t] > 0)
        def _():
            for copy in copies(t):
                copy.start()

        return carry

    lax.fori_loop(0, tiles, start, 0)
    total[...] = jnp.zeros_like(total)
    ids = lax.broadcasted_iota(jnp.int32, (nodes, rows), 0)

    def tile(t, carry):
        @pl.when(live[t] > 0)
        def _():
            turns = SIZES["z"] // span
            y, z = t // turns, lax.rem(t, turns) * span
            senders = jnp.concatenate(
                [
                    jnp.concatenate(
                        [
                            arrived[(((z + n // cores) * cores + n % cores) * FEATS + f) * SIZES["y"] + y]
                            for n in range(GROUP)
                        ],
                        0,
                    )
                    for f in range(FEATS)
                ],
                1,
            )
            parts = [slice(i, i + rows // 2) for i in (0, rows // 2)]
            products = [dot(senders[p], ws[...]) for p in parts]
            for copy in copies(t):
                copy.wait()
            actives = [
                silu(pre_tiles[t, p, :] + product).astype(jnp.bfloat16)
                for p, product in zip(parts, products)
            ]
            updates = [dot(active, w2[...]) + b2[...] for active in actives]
            news = [
                edge_tiles[t, p, :].astype(jnp.float32) + normalize(update, gain[...], shift[...])
                for p, update in zip(parts, updates)
            ]
            new = jnp.concatenate([n.astype(jnp.bfloat16) for n in news], 0)
            sel = (ids == dst_row[t]).astype(jnp.float32).astype(jnp.bfloat16)
            total[...] += dot(sel, new)

        return carry

    lax.fori_loop(0, tiles, tile, 0)
    first[...] = total[: nodes // 2, :].astype(jnp.bfloat16)
    second[...] = total[nodes // 2 :, :].astype(jnp.bfloat16)


def node_kernel(
    column, first, first_got, second, second_got, node_pre, mesh_rows, weights, b2, gain, shift,
    out, full, pre_here, sem,
):
    f32 = jnp.float32
    quarter = out.shape[1]
    width = full.shape[1]
    copy = pltpu.make_async_copy(node_pre, pre_here, sem)
    copy.start()
    summed = jnp.concatenate(
        [
            (u[...].astype(f32) + v[...].astype(f32)).astype(jnp.bfloat16)
            for u, v in ((first, first_got), (second, second_got))
        ],
        0,
    )
    hidden = dot(summed, weights[:width, :])
    copy.wait()
    active = silu(pre_here[...] + hidden).astype(jnp.bfloat16)
    update = dot(active, weights[width:, :]) + b2[...]
    full[...] = mesh_rows[...].astype(f32) + normalize(update, gain[...], shift[...])
    at = pl.ds(pl.multiple_of(column[0] * quarter, quarter), quarter)
    out[...] = full[:, at].astype(jnp.bfloat16)


def body(
    grid_latent,
    mesh_latent,
    edge_latent,
    edge_src,
    edge_dst,
    edge_w1,
    edge_b1,
    edge_w2,
    edge_b2,
    edge_gain,
    edge_shift,
    node_w1,
    node_b1,
    node_w2,
    node_b2,
    node_gain,
    node_shift,
):
    bands = math.prod(SIZES.values())
    feats = FEATS
    quarter = grid_latent.shape[1]
    width = quarter * feats
    nodes = mesh_latent.shape[0]
    row = lambda v: v.reshape(1, -1)

    picked = pick_rows(grid_latent, edge_src.reshape(-1))
    picked = picked.reshape(bands * feats, -1, quarter)
    arrived = lax.all_to_all(picked, ("z", "core", "feat", "y"), 0, 0, tiled=True)

    edges = edge_latent.reshape(-1, width)
    targets = edge_dst.reshape(-1)
    slots = targets.shape[0]
    tiles = bands // GROUP
    live = jnp.any((targets < nodes).reshape(tiles, -1), 1).astype(jnp.int32)
    mesh_rows = lax.all_gather(mesh_latent, "feat", axis=1, tiled=True)

    pre, node_pre = pl.pallas_call(
        early_kernel,
        out_shape=[
            jax.ShapeDtypeStruct((slots, width), jnp.float32),
            jax.ShapeDtypeStruct((nodes, width), jnp.float32),
        ],
        in_specs=[SMEM] + [VMEM] * 7,
        out_specs=[VMEM] * 2,
        cost_estimate=pl.CostEstimate(
            flops=2 * slots * width * width * 2, bytes_accessed=12 << 20, transcendentals=0
        ),
        compiler_params=pltpu.CompilerParams(vmem_limit_bytes=16 << 20),
        name="early",
    )(live, edges, targets.reshape(-1, 1), mesh_rows, edge_w1, row(edge_b1), node_w1, row(node_b1))

    rows = slots // tiles
    first, second = pl.pallas_call(
        late_kernel,
        out_shape=[pltpu.VMEM((nodes // 2, width), jnp.bfloat16)] * 2,
        in_specs=[SMEM, VMEM, HBM, HBM] + [VMEM] * 6,
        out_specs=[VMEM] * 2,
        scratch_shapes=[
            pltpu.VMEM((tiles, rows, width), jnp.bfloat16),
            pltpu.VMEM((tiles, rows, width), jnp.float32),
            pltpu.VMEM((nodes, width), jnp.float32),
            pltpu.SemaphoreType.DMA((2, tiles)),
        ],
        cost_estimate=pl.CostEstimate(
            flops=2 * slots * width * width * 2, bytes_accessed=12 << 20, transcendentals=0
        ),
        compiler_params=pltpu.CompilerParams(vmem_limit_bytes=20 << 20),
        name="late",
    )(
        live,
        in_vmem(arrived),
        in_hbm(edges),
        in_hbm(pre),
        targets.reshape(tiles, 1, -1),
        in_vmem(edge_w1[width : 2 * width]),
        in_vmem(edge_w2),
        row(edge_b2),
        row(edge_gain),
        row(edge_shift),
    )

    pairing = [(i, i ^ 1) for i in range(feats)]
    crossing = [(i, feats - 1 - i) for i in range(feats)]
    first_got = lax.ppermute(first, "feat", pairing)
    second_got = lax.ppermute(second, "feat", crossing)
    add = lambda u, v: (u.astype(jnp.float32) + v.astype(jnp.float32)).astype(jnp.bfloat16)
    first = add(first, first_got)
    second = add(second, second_got)
    first_got = lax.ppermute(first, "feat", crossing)
    second_got = lax.ppermute(second, "feat", pairing)
    column = jnp.full((1,), lax.axis_index("feat"), jnp.int32)
    return pl.pallas_call(
        node_kernel,
        out_shape=jax.ShapeDtypeStruct((nodes, quarter), jnp.bfloat16),
        in_specs=[SMEM] + [VMEM] * 4 + [HBM] + [VMEM] * 5,
        out_specs=VMEM,
        scratch_shapes=[
            pltpu.VMEM((nodes, width), jnp.float32),
            pltpu.VMEM((nodes, width), jnp.float32),
            pltpu.SemaphoreType.DMA,
        ],
        compiler_params=pltpu.CompilerParams(vmem_limit_bytes=8 << 20),
        name="node",
    )(
        column,
        first,
        first_got,
        second,
        second_got,
        in_hbm(node_pre),
        mesh_rows,
        jnp.concatenate([node_w1[width:], node_w2], 0),
        row(node_b2),
        row(node_gain),
        row(node_shift),
    )


def solution(mesh):
    parts = jax.sharding.Mesh(
        mesh.devices.reshape(*SIZES.values(), FEATS), BAND + ("feat",), axis_types=(AUTO,) * 4
    )
    placed = (
        P(BAND, "feat"),
        P(BAND, "feat"),
        P(BAND, "feat", None, None),
        P(BAND, None),
        P(BAND, "feat", None),
    ) + (P(),) * 12
    return jax.shard_map(
        body, mesh=parts, in_specs=placed, out_specs=P(BAND, "feat"), check_vma=False
    )
```

```python
import math

import jax
import jax.numpy as jnp
from jax import lax
from jax.experimental import pallas as pl
from jax.experimental.pallas import tpu as pltpu
from jax.sharding import PartitionSpec as P

EPSILON = 1e-05
SIZES = {"y": 4, "z": 8, "core": 2}
FEATS = 4
SLOTS = 32
BAND = tuple(SIZES)
GROUP = 8
VMEM = pl.BlockSpec(memory_space=pltpu.VMEM)
SMEM = pl.BlockSpec(memory_space=pltpu.SMEM)
HBM = pl.BlockSpec(memory_space=pltpu.HBM)
ANY = pl.BlockSpec(memory_space=pl.ANY)
AUTO = jax.sharding.AxisType.Auto


def in_vmem(value):
    return pltpu.with_memory_space_constraint(value, pltpu.VMEM)


def dot(a, b):
    return jnp.dot(a, b, preferred_element_type=jnp.float32)


def in_hbm(value):
    return pltpu.with_memory_space_constraint(value, pltpu.HBM)


def silu(v):
    return v / (1.0 + jnp.exp(-v))


def normalize(values, gain, shift):
    average = jnp.mean(values, -1, keepdims=True)
    centered = values - average
    variance = jnp.mean(centered * centered, -1, keepdims=True)
    return centered * lax.rsqrt(variance + EPSILON) * gain + shift


def pick_kernel(ids, ids_row, table, held, wide, pairs, rows):
    half = table.shape[0] // 2
    count = FEATS * SLOTS
    sends = SIZES["y"] * SIZES["core"]
    step = sends * count
    pieces = sends // 2
    per = (step - pieces * count) // (pieces * (half // 256))
    wide[...] = table[...].astype(jnp.float32)
    pairs[...] = jnp.concatenate([table[:half], table[half:]], 1)
    lane = lax.broadcasted_iota(jnp.int32, (count, 128), 1)

    def band_of(n):
        y, core = divmod(n, SIZES["core"])
        return y * SIZES["z"] * SIZES["core"] + core

    def put(n, z, value):
        y, core = divmod(n, SIZES["core"])
        for f in range(FEATS):
            place = ((core * FEATS + f) * SIZES["y"] + y) * SLOTS
            held[pl.ds(pl.multiple_of(z * step + place, SLOTS), SLOTS), :] = value[f * SLOTS : (f + 1) * SLOTS]

    def one_z(z, carry):
        r = 0
        first_band = z * SIZES["core"]
        base = first_band * count
        for g in range(pieces):
            want = jnp.broadcast_to(ids_row[first_band + band_of(g)], (128, 128)).T
            upper = want >= half
            place = jnp.where(upper, want - half, want)
            both = None
            for j in range(half // 256):
                onehot = jnp.concatenate(
                    [
                        jnp.where(place == lane + (256 * j + 128 * u), 1.0, 0.0).astype(jnp.bfloat16)
                        for u in range(2)
                    ],
                    1,
                )
                part = dot(onehot, pairs[256 * j : 256 * (j + 1), :])
                both = part if both is None else both + part
                for _ in range(per):
                    n, slot = divmod(r, count)
                    rows[pl.ds(r, 1), :] = wide[pl.ds(ids[base + (band_of(pieces + n) * count + slot)], 1), :]
                    r += 1
            put(g, z, jnp.where(upper, both[:, 128:], both[:, :128]).astype(jnp.bfloat16))
        for n in range(pieces):
            put(pieces + n, z, rows[n * count : (n + 1) * count, :].astype(jnp.bfloat16))
        return carry

    lax.fori_loop(0, SIZES["z"], one_z, 0)


def pick_rows(table, ids):
    height, width = table.shape
    per_turn = SIZES["y"] * SIZES["core"] * FEATS * SLOTS
    return pl.pallas_call(
        pick_kernel,
        out_shape=jax.ShapeDtypeStruct((ids.shape[0], width), jnp.bfloat16),
        in_specs=[SMEM, VMEM, VMEM],
        out_specs=VMEM,
        scratch_shapes=[
            pltpu.VMEM((height, width), jnp.float32),
            pltpu.VMEM((height // 2, 2 * width), jnp.bfloat16),
            pltpu.VMEM((per_turn // 2, width), jnp.float32),
        ],
        name="pick_rows",
    )(ids, ids.reshape(-1, 1, 128), table)


def early_kernel(live, edges, dst_col, mesh_rows, w1, b1, nw1, nb1, pre, node_pre):
    width = edges.shape[1]
    nodes = mesh_rows.shape[0]
    tiles = live.shape[0]
    rows = edges.shape[0] // tiles
    node_pre[...] = dot(mesh_rows[...], nw1[:width, :]) + nb1[...]
    projected = dot(mesh_rows[...], w1[2 * width :, :]) + b1[...]
    high = projected.astype(jnp.bfloat16)
    low = (projected - high.astype(jnp.float32)).astype(jnp.bfloat16)
    ids = lax.broadcasted_iota(jnp.int32, (rows, nodes), 1)

    def tile(t, carry):
        @pl.when(live[t] > 0)
        def _():
            at = pl.ds(pl.multiple_of(t * rows, rows), rows)
            pick = (ids == dst_col[at, :]).astype(jnp.float32).astype(jnp.bfloat16)
            pre[at, :] = dot(edges[at, :], w1[:width, :]) + (dot(pick, high) + dot(pick, low))

        return carry

    lax.fori_loop(0, tiles, tile, 0)


def late_kernel(
    live, arrived, edges, pre, dst_row, ws, w2, b2, gain, shift,
    first, second, edge_tiles, pre_tiles, products, total, sems,
):
    width = ws.shape[0]
    nodes = total.shape[0]
    tiles, rows = edge_tiles.shape[:2]
    cores = SIZES["core"]
    span = GROUP // cores

    def copies(t):
        at = pl.ds(pl.multiple_of(t * rows, rows), rows)
        return (
            pltpu.make_async_copy(pre.at[at], pre_tiles.at[t], sems.at[0, t]),
            pltpu.make_async_copy(edges.at[at], edge_tiles.at[t], sems.at[1, t]),
        )

    def start(t, carry):
        @pl.when(live[t] > 0)
        def _():
            for copy in copies(t):
                copy.start()

        return carry

    lax.fori_loop(0, tiles, start, 0)
    total[...] = jnp.zeros_like(total)
    ids = lax.broadcasted_iota(jnp.int32, (nodes, rows), 0)

    def product(t, carry):
        @pl.when(live[t] > 0)
        def _():
            turns = SIZES["z"] // span
            y, z = t // turns, lax.rem(t, turns) * span
            senders = jnp.concatenate(
                [
                    jnp.concatenate(
                        [
                            arrived[(((z + n // cores) * cores + n % cores) * FEATS + f) * SIZES["y"] + y]
                            for n in range(GROUP)
                        ],
                        0,
                    )
                    for f in range(FEATS)
                ],
                1,
            )
            products[t] = dot(senders, ws[...])

        return carry

    lax.fori_loop(0, tiles, product, 0)

    def tile(t, carry):
        @pl.when(live[t] > 0)
        def _():
            parts = [slice(i, i + rows // 2) for i in (0, rows // 2)]
            for copy in copies(t):
                copy.wait()
            actives = [
                silu(pre_tiles[t, p, :] + products[t, p, :]).astype(jnp.bfloat16) for p in parts
            ]
            updates = [dot(active, w2[...]) + b2[...] for active in actives]
            news = [
                edge_tiles[t, p, :].astype(jnp.float32) + normalize(update, gain[...], shift[...])
                for p, update in zip(parts, updates)
            ]
            new = jnp.concatenate([n.astype(jnp.bfloat16) for n in news], 0)
            sel = (ids == dst_row[t]).astype(jnp.float32).astype(jnp.bfloat16)
            total[...] += dot(sel, new)

        return carry

    lax.fori_loop(0, tiles, tile, 0)
    first[...] = total[: nodes // 2, :].astype(jnp.bfloat16)
    second[...] = total[nodes // 2 :, :].astype(jnp.bfloat16)


def node_kernel(
    column, first, first_got, second, second_got, node_pre, mesh_rows, weights, b2, gain, shift,
    out, full, pre_here, sem,
):
    f32 = jnp.float32
    quarter = out.shape[1]
    width = full.shape[1]
    copy = pltpu.make_async_copy(node_pre, pre_here, sem)
    copy.start()
    summed = jnp.concatenate(
        [
            (u[...].astype(f32) + v[...].astype(f32)).astype(jnp.bfloat16)
            for u, v in ((first, first_got), (second, second_got))
        ],
        0,
    )
    hidden = dot(summed, weights[:width, :])
    copy.wait()
    active = silu(pre_here[...] + hidden).astype(jnp.bfloat16)
    update = dot(active, weights[width:, :]) + b2[...]
    full[...] = mesh_rows[...].astype(f32) + normalize(update, gain[...], shift[...])
    at = pl.ds(pl.multiple_of(column[0] * quarter, quarter), quarter)
    out[...] = full[:, at].astype(jnp.bfloat16)


def body(
    grid_latent,
    mesh_latent,
    edge_latent,
    edge_src,
    edge_dst,
    edge_w1,
    edge_b1,
    edge_w2,
    edge_b2,
    edge_gain,
    edge_shift,
    node_w1,
    node_b1,
    node_w2,
    node_b2,
    node_gain,
    node_shift,
):
    bands = math.prod(SIZES.values())
    feats = FEATS
    quarter = grid_latent.shape[1]
    width = quarter * feats
    nodes = mesh_latent.shape[0]
    row = lambda v: v.reshape(1, -1)

    picked = pick_rows(grid_latent, edge_src.reshape(-1))
    picked = picked.reshape(bands * feats, -1, quarter)
    arrived = lax.all_to_all(picked, ("z", "core", "feat", "y"), 0, 0, tiled=True)

    edges = edge_latent.reshape(-1, width)
    targets = edge_dst.reshape(-1)
    slots = targets.shape[0]
    tiles = bands // GROUP
    live = jnp.any((targets < nodes).reshape(tiles, -1), 1).astype(jnp.int32)
    mesh_rows = lax.all_gather(mesh_latent, "feat", axis=1, tiled=True)

    pre, node_pre = pl.pallas_call(
        early_kernel,
        out_shape=[
            jax.ShapeDtypeStruct((slots, width), jnp.float32),
            jax.ShapeDtypeStruct((nodes, width), jnp.float32),
        ],
        in_specs=[SMEM] + [VMEM] * 7,
        out_specs=[VMEM] * 2,
        cost_estimate=pl.CostEstimate(
            flops=2 * slots * width * width * 2, bytes_accessed=12 << 20, transcendentals=0
        ),
        compiler_params=pltpu.CompilerParams(vmem_limit_bytes=16 << 20),
        name="early",
    )(live, edges, targets.reshape(-1, 1), mesh_rows, edge_w1, row(edge_b1), node_w1, row(node_b1))

    rows = slots // tiles
    first, second = pl.pallas_call(
        late_kernel,
        out_shape=[pltpu.VMEM((nodes // 2, width), jnp.bfloat16)] * 2,
        in_specs=[SMEM, VMEM, HBM, HBM] + [VMEM] * 6,
        out_specs=[VMEM] * 2,
        scratch_shapes=[
            pltpu.VMEM((tiles, rows, width), jnp.bfloat16),
            pltpu.VMEM((tiles, rows, width), jnp.float32),
            pltpu.VMEM((tiles, rows, width), jnp.float32),
            pltpu.VMEM((nodes, width), jnp.float32),
            pltpu.SemaphoreType.DMA((2, tiles)),
        ],
        cost_estimate=pl.CostEstimate(
            flops=2 * slots * width * width * 2, bytes_accessed=12 << 20, transcendentals=0
        ),
        compiler_params=pltpu.CompilerParams(vmem_limit_bytes=20 << 20),
        name="late",
    )(
        live,
        in_vmem(arrived),
        in_hbm(edges),
        in_hbm(pre),
        targets.reshape(tiles, 1, -1),
        in_vmem(edge_w1[width : 2 * width]),
        in_vmem(edge_w2),
        row(edge_b2),
        row(edge_gain),
        row(edge_shift),
    )

    pairing = [(i, i ^ 1) for i in range(feats)]
    crossing = [(i, feats - 1 - i) for i in range(feats)]
    first_got = lax.ppermute(first, "feat", pairing)
    second_got = lax.ppermute(second, "feat", crossing)
    add = lambda u, v: (u.astype(jnp.float32) + v.astype(jnp.float32)).astype(jnp.bfloat16)
    first = add(first, first_got)
    second = add(second, second_got)
    first_got = lax.ppermute(first, "feat", crossing)
    second_got = lax.ppermute(second, "feat", pairing)
    column = jnp.full((1,), lax.axis_index("feat"), jnp.int32)
    return pl.pallas_call(
        node_kernel,
        out_shape=jax.ShapeDtypeStruct((nodes, quarter), jnp.bfloat16),
        in_specs=[SMEM] + [VMEM] * 4 + [HBM] + [VMEM] * 5,
        out_specs=VMEM,
        scratch_shapes=[
            pltpu.VMEM((nodes, width), jnp.float32),
            pltpu.VMEM((nodes, width), jnp.float32),
            pltpu.SemaphoreType.DMA,
        ],
        compiler_params=pltpu.CompilerParams(vmem_limit_bytes=8 << 20),
        name="node",
    )(
        column,
        first,
        first_got,
        second,
        second_got,
        in_hbm(node_pre),
        mesh_rows,
        jnp.concatenate([node_w1[width:], node_w2], 0),
        row(node_b2),
        row(node_gain),
        row(node_shift),
    )


def solution(mesh):
    parts = jax.sharding.Mesh(
        mesh.devices.reshape(*SIZES.values(), FEATS), BAND + ("feat",), axis_types=(AUTO,) * 4
    )
    placed = (
        P(BAND, "feat"),
        P(BAND, "feat"),
        P(BAND, "feat", None, None),
        P(BAND, None),
        P(BAND, "feat", None),
    ) + (P(),) * 12
    return jax.shard_map(
        body, mesh=parts, in_specs=placed, out_specs=P(BAND, "feat"), check_vma=False
    )
```

```python
import math

import jax
import jax.numpy as jnp
from jax import lax
from jax.experimental import pallas as pl
from jax.experimental.pallas import tpu as pltpu
from jax.sharding import PartitionSpec as P

EPSILON = 1e-05
SIZES = {"y": 4, "z": 8, "core": 2}
FEATS = 4
SLOTS = 32
BAND = tuple(SIZES)
GROUP = 4
VMEM = pl.BlockSpec(memory_space=pltpu.VMEM)
SMEM = pl.BlockSpec(memory_space=pltpu.SMEM)
HBM = pl.BlockSpec(memory_space=pltpu.HBM)
ANY = pl.BlockSpec(memory_space=pl.ANY)
AUTO = jax.sharding.AxisType.Auto


def in_vmem(value):
    return pltpu.with_memory_space_constraint(value, pltpu.VMEM)


def dot(a, b):
    return jnp.dot(a, b, preferred_element_type=jnp.float32)


def in_hbm(value):
    return pltpu.with_memory_space_constraint(value, pltpu.HBM)


def silu(v):
    return v / (1.0 + jnp.exp(-v))


def normalize(values, gain, shift):
    average = jnp.mean(values, -1, keepdims=True)
    centered = values - average
    variance = jnp.mean(centered * centered, -1, keepdims=True)
    return centered * lax.rsqrt(variance + EPSILON) * gain + shift


def pick_kernel(ids, ids_row, table, held, wide, pairs, rows):
    half = table.shape[0] // 2
    count = FEATS * SLOTS
    sends = SIZES["y"] * SIZES["core"]
    step = sends * count
    pieces = sends // 2
    per = (step - pieces * count) // (pieces * (half // 256))
    wide[...] = table[...].astype(jnp.float32)
    pairs[...] = jnp.concatenate([table[:half], table[half:]], 1)
    lane = lax.broadcasted_iota(jnp.int32, (count, 128), 1)

    def band_of(n):
        y, core = divmod(n, SIZES["core"])
        return y * SIZES["z"] * SIZES["core"] + core

    def put(n, z, value):
        y, core = divmod(n, SIZES["core"])
        for f in range(FEATS):
            place = ((core * FEATS + f) * SIZES["y"] + y) * SLOTS
            held[pl.ds(pl.multiple_of(z * step + place, SLOTS), SLOTS), :] = value[f * SLOTS : (f + 1) * SLOTS]

    def one_z(z, carry):
        r = 0
        first_band = z * SIZES["core"]
        base = first_band * count
        for g in range(pieces):
            want = jnp.broadcast_to(ids_row[first_band + band_of(g)], (128, 128)).T
            upper = want >= half
            place = jnp.where(upper, want - half, want)
            both = None
            for j in range(half // 256):
                onehot = jnp.concatenate(
                    [
                        jnp.where(place == lane + (256 * j + 128 * u), 1.0, 0.0).astype(jnp.bfloat16)
                        for u in range(2)
                    ],
                    1,
                )
                part = dot(onehot, pairs[256 * j : 256 * (j + 1), :])
                both = part if both is None else both + part
                for _ in range(per):
                    n, slot = divmod(r, count)
                    rows[pl.ds(r, 1), :] = wide[pl.ds(ids[base + (band_of(pieces + n) * count + slot)], 1), :]
                    r += 1
            put(g, z, jnp.where(upper, both[:, 128:], both[:, :128]).astype(jnp.bfloat16))
        for n in range(pieces):
            put(pieces + n, z, rows[n * count : (n + 1) * count, :].astype(jnp.bfloat16))
        return carry

    lax.fori_loop(0, SIZES["z"], one_z, 0)


def pick_rows(table, ids):
    height, width = table.shape
    per_turn = SIZES["y"] * SIZES["core"] * FEATS * SLOTS
    return pl.pallas_call(
        pick_kernel,
        out_shape=jax.ShapeDtypeStruct((ids.shape[0], width), jnp.bfloat16),
        in_specs=[SMEM, VMEM, VMEM],
        out_specs=VMEM,
        scratch_shapes=[
            pltpu.VMEM((height, width), jnp.float32),
            pltpu.VMEM((height // 2, 2 * width), jnp.bfloat16),
            pltpu.VMEM((per_turn // 2, width), jnp.float32),
        ],
        name="pick_rows",
    )(ids, ids.reshape(-1, 1, 128), table)


def early_kernel(live, edges, dst_col, mesh_rows, w1, b1, nw1, nb1, pre, node_pre):
    width = edges.shape[1]
    nodes = mesh_rows.shape[0]
    tiles = live.shape[0]
    rows = edges.shape[0] // tiles
    node_pre[...] = dot(mesh_rows[...], nw1[:width, :]) + nb1[...]
    projected = dot(mesh_rows[...], w1[2 * width :, :]) + b1[...]
    high = projected.astype(jnp.bfloat16)
    low = (projected - high.astype(jnp.float32)).astype(jnp.bfloat16)
    ids = lax.broadcasted_iota(jnp.int32, (rows, nodes), 1)

    def tile(t, carry):
        @pl.when(live[t] > 0)
        def _():
            at = pl.ds(pl.multiple_of(t * rows, rows), rows)
            pick = (ids == dst_col[at, :]).astype(jnp.float32).astype(jnp.bfloat16)
            pre[at, :] = dot(edges[at, :], w1[:width, :]) + (dot(pick, high) + dot(pick, low))

        return carry

    lax.fori_loop(0, tiles, tile, 0)


def late_kernel(
    live, arrived, edges, pre, dst_row, ws, w2, b2, gain, shift,
    first, second, edge_tiles, pre_tiles, products, total, sems,
):
    width = ws.shape[0]
    nodes = total.shape[0]
    tiles, rows = edge_tiles.shape[:2]
    cores = SIZES["core"]
    span = GROUP // cores

    def copies(t):
        at = pl.ds(pl.multiple_of(t * rows, rows), rows)
        return (
            pltpu.make_async_copy(pre.at[at], pre_tiles.at[t], sems.at[0, t]),
            pltpu.make_async_copy(edges.at[at], edge_tiles.at[t], sems.at[1, t]),
        )

    def start(t, carry):
        @pl.when(live[t] > 0)
        def _():
            for copy in copies(t):
                copy.start()

        return carry

    lax.fori_loop(0, tiles, start, 0)
    total[...] = jnp.zeros_like(total)
    ids = lax.broadcasted_iota(jnp.int32, (nodes, rows), 0)

    def product(t, carry):
        @pl.when(live[t] > 0)
        def _():
            turns = SIZES["z"] // span
            y, z = t // turns, lax.rem(t, turns) * span
            senders = jnp.concatenate(
                [
                    jnp.concatenate(
                        [
                            arrived[(((z + n // cores) * cores + n % cores) * FEATS + f) * SIZES["y"] + y]
                            for n in range(GROUP)
                        ],
                        0,
                    )
                    for f in range(FEATS)
                ],
                1,
            )
            products[t] = dot(senders, ws[...])

        return carry

    lax.fori_loop(0, tiles, product, 0)

    def tile(t, carry):
        @pl.when(live[t] > 0)
        def _():
            parts = [slice(0, rows)]
            for copy in copies(t):
                copy.wait()
            actives = [
                silu(pre_tiles[t, p, :] + products[t, p, :]).astype(jnp.bfloat16) for p in parts
            ]
            updates = [dot(active, w2[...]) + b2[...] for active in actives]
            news = [
                edge_tiles[t, p, :].astype(jnp.float32) + normalize(update, gain[...], shift[...])
                for p, update in zip(parts, updates)
            ]
            new = jnp.concatenate([n.astype(jnp.bfloat16) for n in news], 0)
            sel = (ids == dst_row[t]).astype(jnp.float32).astype(jnp.bfloat16)
            total[...] += dot(sel, new)

        return carry

    lax.fori_loop(0, tiles, tile, 0)
    first[...] = total[: nodes // 2, :].astype(jnp.bfloat16)
    second[...] = total[nodes // 2 :, :].astype(jnp.bfloat16)


def node_kernel(
    column, first, first_got, second, second_got, node_pre, mesh_rows, weights, b2, gain, shift,
    out, full, pre_here, sem,
):
    f32 = jnp.float32
    quarter = out.shape[1]
    width = full.shape[1]
    copy = pltpu.make_async_copy(node_pre, pre_here, sem)
    copy.start()
    summed = jnp.concatenate(
        [
            (u[...].astype(f32) + v[...].astype(f32)).astype(jnp.bfloat16)
            for u, v in ((first, first_got), (second, second_got))
        ],
        0,
    )
    hidden = dot(summed, weights[:width, :])
    copy.wait()
    active = silu(pre_here[...] + hidden).astype(jnp.bfloat16)
    update = dot(active, weights[width:, :]) + b2[...]
    full[...] = mesh_rows[...].astype(f32) + normalize(update, gain[...], shift[...])
    at = pl.ds(pl.multiple_of(column[0] * quarter, quarter), quarter)
    out[...] = full[:, at].astype(jnp.bfloat16)


def body(
    grid_latent,
    mesh_latent,
    edge_latent,
    edge_src,
    edge_dst,
    edge_w1,
    edge_b1,
    edge_w2,
    edge_b2,
    edge_gain,
    edge_shift,
    node_w1,
    node_b1,
    node_w2,
    node_b2,
    node_gain,
    node_shift,
):
    bands = math.prod(SIZES.values())
    feats = FEATS
    quarter = grid_latent.shape[1]
    width = quarter * feats
    nodes = mesh_latent.shape[0]
    row = lambda v: v.reshape(1, -1)

    picked = pick_rows(grid_latent, edge_src.reshape(-1))
    picked = picked.reshape(bands * feats, -1, quarter)
    arrived = lax.all_to_all(picked, ("z", "core", "feat", "y"), 0, 0, tiled=True)

    edges = edge_latent.reshape(-1, width)
    targets = edge_dst.reshape(-1)
    slots = targets.shape[0]
    tiles = bands // GROUP
    live = jnp.any((targets < nodes).reshape(tiles, -1), 1).astype(jnp.int32)
    mesh_rows = lax.all_gather(mesh_latent, "feat", axis=1, tiled=True)

    pre, node_pre = pl.pallas_call(
        early_kernel,
        out_shape=[
            jax.ShapeDtypeStruct((slots, width), jnp.float32),
            jax.ShapeDtypeStruct((nodes, width), jnp.float32),
        ],
        in_specs=[SMEM] + [VMEM] * 7,
        out_specs=[VMEM] * 2,
        cost_estimate=pl.CostEstimate(
            flops=2 * slots * width * width * 2, bytes_accessed=12 << 20, transcendentals=0
        ),
        compiler_params=pltpu.CompilerParams(vmem_limit_bytes=16 << 20),
        name="early",
    )(live, edges, targets.reshape(-1, 1), mesh_rows, edge_w1, row(edge_b1), node_w1, row(node_b1))

    rows = slots // tiles
    first, second = pl.pallas_call(
        late_kernel,
        out_shape=[pltpu.VMEM((nodes // 2, width), jnp.bfloat16)] * 2,
        in_specs=[SMEM, VMEM, HBM, HBM] + [VMEM] * 6,
        out_specs=[VMEM] * 2,
        scratch_shapes=[
            pltpu.VMEM((tiles, rows, width), jnp.bfloat16),
            pltpu.VMEM((tiles, rows, width), jnp.float32),
            pltpu.VMEM((tiles, rows, width), jnp.float32),
            pltpu.VMEM((nodes, width), jnp.float32),
            pltpu.SemaphoreType.DMA((2, tiles)),
        ],
        cost_estimate=pl.CostEstimate(
            flops=2 * slots * width * width * 2, bytes_accessed=12 << 20, transcendentals=0
        ),
        compiler_params=pltpu.CompilerParams(vmem_limit_bytes=20 << 20),
        name="late",
    )(
        live,
        in_vmem(arrived),
        in_hbm(edges),
        in_hbm(pre),
        targets.reshape(tiles, 1, -1),
        in_vmem(edge_w1[width : 2 * width]),
        in_vmem(edge_w2),
        row(edge_b2),
        row(edge_gain),
        row(edge_shift),
    )

    pairing = [(i, i ^ 1) for i in range(feats)]
    crossing = [(i, feats - 1 - i) for i in range(feats)]
    first_got = lax.ppermute(first, "feat", pairing)
    second_got = lax.ppermute(second, "feat", crossing)
    add = lambda u, v: (u.astype(jnp.float32) + v.astype(jnp.float32)).astype(jnp.bfloat16)
    first = add(first, first_got)
    second = add(second, second_got)
    first_got = lax.ppermute(first, "feat", crossing)
    second_got = lax.ppermute(second, "feat", pairing)
    column = jnp.full((1,), lax.axis_index("feat"), jnp.int32)
    return pl.pallas_call(
        node_kernel,
        out_shape=jax.ShapeDtypeStruct((nodes, quarter), jnp.bfloat16),
        in_specs=[SMEM] + [VMEM] * 4 + [HBM] + [VMEM] * 5,
        out_specs=VMEM,
        scratch_shapes=[
            pltpu.VMEM((nodes, width), jnp.float32),
            pltpu.VMEM((nodes, width), jnp.float32),
            pltpu.SemaphoreType.DMA,
        ],
        compiler_params=pltpu.CompilerParams(vmem_limit_bytes=8 << 20),
        name="node",
    )(
        column,
        first,
        first_got,
        second,
        second_got,
        in_hbm(node_pre),
        mesh_rows,
        jnp.concatenate([node_w1[width:], node_w2], 0),
        row(node_b2),
        row(node_gain),
        row(node_shift),
    )


def solution(mesh):
    parts = jax.sharding.Mesh(
        mesh.devices.reshape(*SIZES.values(), FEATS), BAND + ("feat",), axis_types=(AUTO,) * 4
    )
    placed = (
        P(BAND, "feat"),
        P(BAND, "feat"),
        P(BAND, "feat", None, None),
        P(BAND, None),
        P(BAND, "feat", None),
    ) + (P(),) * 12
    return jax.shard_map(
        body, mesh=parts, in_specs=placed, out_specs=P(BAND, "feat"), check_vma=False
    )
```

```python
import math

import jax
import jax.numpy as jnp
from jax import lax
from jax.experimental import pallas as pl
from jax.experimental.pallas import tpu as pltpu
from jax.sharding import PartitionSpec as P

EPSILON = 1e-05
SIZES = {"y": 4, "z": 8, "core": 2}
FEATS = 4
SLOTS = 32
BAND = tuple(SIZES)
GROUP = 8
VMEM = pl.BlockSpec(memory_space=pltpu.VMEM)
SMEM = pl.BlockSpec(memory_space=pltpu.SMEM)
HBM = pl.BlockSpec(memory_space=pltpu.HBM)
ANY = pl.BlockSpec(memory_space=pl.ANY)
AUTO = jax.sharding.AxisType.Auto


def in_vmem(value):
    return pltpu.with_memory_space_constraint(value, pltpu.VMEM)


def dot(a, b):
    return jnp.dot(a, b, preferred_element_type=jnp.float32)


def in_hbm(value):
    return pltpu.with_memory_space_constraint(value, pltpu.HBM)


def silu(v):
    return v / (1.0 + jnp.exp(-v))


def normalize(values, gain, shift):
    average = jnp.mean(values, -1, keepdims=True)
    centered = values - average
    variance = jnp.mean(centered * centered, -1, keepdims=True)
    return centered * lax.rsqrt(variance + EPSILON) * gain + shift


def pick_kernel(ids, ids_row, table, held, wide, pairs, rows):
    half = table.shape[0] // 2
    count = FEATS * SLOTS
    sends = SIZES["y"] * SIZES["core"]
    step = sends * count
    pieces = sends // 2
    per = (step - pieces * count) // (pieces * (half // 256))
    wide[...] = table[...].astype(jnp.float32)
    pairs[...] = jnp.concatenate([table[:half], table[half:]], 1)
    lane = lax.broadcasted_iota(jnp.int32, (count, 128), 1)

    def band_of(n):
        y, core = divmod(n, SIZES["core"])
        return y * SIZES["z"] * SIZES["core"] + core

    def put(n, z, value):
        y, core = divmod(n, SIZES["core"])
        for f in range(FEATS):
            place = ((core * FEATS + f) * SIZES["y"] + y) * SLOTS
            held[pl.ds(pl.multiple_of(z * step + place, SLOTS), SLOTS), :] = value[f * SLOTS : (f + 1) * SLOTS]

    def one_z(z, carry):
        r = 0
        first_band = z * SIZES["core"]
        base = first_band * count
        for g in range(pieces):
            want = jnp.broadcast_to(ids_row[first_band + band_of(g)], (128, 128)).T
            upper = want >= half
            place = jnp.where(upper, want - half, want)
            both = None
            for j in range(half // 256):
                onehot = jnp.concatenate(
                    [
                        jnp.where(place == lane + (256 * j + 128 * u), 1.0, 0.0).astype(jnp.bfloat16)
                        for u in range(2)
                    ],
                    1,
                )
                part = dot(onehot, pairs[256 * j : 256 * (j + 1), :])
                both = part if both is None else both + part
                for _ in range(per):
                    n, slot = divmod(r, count)
                    rows[pl.ds(r, 1), :] = wide[pl.ds(ids[base + (band_of(pieces + n) * count + slot)], 1), :]
                    r += 1
            put(g, z, jnp.where(upper, both[:, 128:], both[:, :128]).astype(jnp.bfloat16))
        for n in range(pieces):
            put(pieces + n, z, rows[n * count : (n + 1) * count, :].astype(jnp.bfloat16))
        return carry

    lax.fori_loop(0, SIZES["z"], one_z, 0)


def pick_rows(table, ids):
    height, width = table.shape
    per_turn = SIZES["y"] * SIZES["core"] * FEATS * SLOTS
    return pl.pallas_call(
        pick_kernel,
        out_shape=jax.ShapeDtypeStruct((ids.shape[0], width), jnp.bfloat16),
        in_specs=[SMEM, VMEM, VMEM],
        out_specs=VMEM,
        scratch_shapes=[
            pltpu.VMEM((height, width), jnp.float32),
            pltpu.VMEM((height // 2, 2 * width), jnp.bfloat16),
            pltpu.VMEM((per_turn // 2, width), jnp.float32),
        ],
        name="pick_rows",
    )(ids, ids.reshape(-1, 1, 128), table)


def early_kernel(live, edges, dst_col, mesh_rows, w1, b1, nw1, nb1, pre, node_pre):
    width = edges.shape[1]
    nodes = mesh_rows.shape[0]
    tiles = live.shape[0]
    rows = edges.shape[0] // tiles
    node_pre[...] = dot(mesh_rows[...], nw1[:width, :]) + nb1[...]
    projected = dot(mesh_rows[...], w1[2 * width :, :]) + b1[...]
    high = projected.astype(jnp.bfloat16)
    low = (projected - high.astype(jnp.float32)).astype(jnp.bfloat16)
    ids = lax.broadcasted_iota(jnp.int32, (rows, nodes), 1)

    def tile(t, carry):
        @pl.when(live[t] > 0)
        def _():
            at = pl.ds(pl.multiple_of(t * rows, rows), rows)
            pick = (ids == dst_col[at, :]).astype(jnp.float32).astype(jnp.bfloat16)
            pre[at, :] = dot(edges[at, :], w1[:width, :]) + (dot(pick, high) + dot(pick, low))

        return carry

    lax.fori_loop(0, tiles, tile, 0)


def late_kernel(
    live, arrived, edges, pre, dst_row, ws, w2, b2, gain, shift,
    first, second, edge_tiles, pre_tiles, products, total, sems,
):
    width = ws.shape[0]
    nodes = total.shape[0]
    tiles, rows = edge_tiles.shape[:2]
    cores = SIZES["core"]
    span = GROUP // cores

    def copies(t):
        at = pl.ds(pl.multiple_of(t * rows, rows), rows)
        return (
            pltpu.make_async_copy(pre.at[at], pre_tiles.at[t], sems.at[0, t]),
            pltpu.make_async_copy(edges.at[at], edge_tiles.at[t], sems.at[1, t]),
        )

    def start(t, carry):
        @pl.when(live[t] > 0)
        def _():
            for copy in copies(t):
                copy.start()

        return carry

    lax.fori_loop(0, tiles, start, 0)
    total[...] = jnp.zeros_like(total)
    ids = lax.broadcasted_iota(jnp.int32, (nodes, rows), 0)

    def product(t, carry):
        @pl.when(live[t] > 0)
        def _():
            turns = SIZES["z"] // span
            y, z = t // turns, lax.rem(t, turns) * span
            senders = jnp.concatenate(
                [
                    jnp.concatenate(
                        [
                            arrived[(((z + n // cores) * cores + n % cores) * FEATS + f) * SIZES["y"] + y]
                            for n in range(GROUP)
                        ],
                        0,
                    )
                    for f in range(FEATS)
                ],
                1,
            )
            products[t] = dot(senders, ws[...])

        return carry

    lax.fori_loop(0, tiles, product, 0)

    def tile(t, carry):
        @pl.when(live[t] > 0)
        def _():
            parts = [slice(0, rows)]
            for copy in copies(t):
                copy.wait()
            actives = [
                silu(pre_tiles[t, p, :] + products[t, p, :]).astype(jnp.bfloat16) for p in parts
            ]
            updates = [dot(active, w2[...]) + b2[...] for active in actives]
            news = [
                edge_tiles[t, p, :].astype(jnp.float32) + normalize(update, gain[...], shift[...])
                for p, update in zip(parts, updates)
            ]
            new = jnp.concatenate([n.astype(jnp.bfloat16) for n in news], 0)
            sel = (ids == dst_row[t]).astype(jnp.float32).astype(jnp.bfloat16)
            total[...] += dot(sel, new)

        return carry

    lax.fori_loop(0, tiles, tile, 0)
    first[...] = total[: nodes // 2, :].astype(jnp.bfloat16)
    second[...] = total[nodes // 2 :, :].astype(jnp.bfloat16)


def node_kernel(
    column, first, first_got, second, second_got, node_pre, mesh_rows, weights, b2, gain, shift,
    out, full, pre_here, sem,
):
    f32 = jnp.float32
    quarter = out.shape[1]
    width = full.shape[1]
    copy = pltpu.make_async_copy(node_pre, pre_here, sem)
    copy.start()
    summed = jnp.concatenate(
        [
            (u[...].astype(f32) + v[...].astype(f32)).astype(jnp.bfloat16)
            for u, v in ((first, first_got), (second, second_got))
        ],
        0,
    )
    hidden = dot(summed, weights[:width, :])
    copy.wait()
    active = silu(pre_here[...] + hidden).astype(jnp.bfloat16)
    update = dot(active, weights[width:, :]) + b2[...]
    full[...] = mesh_rows[...].astype(f32) + normalize(update, gain[...], shift[...])
    at = pl.ds(pl.multiple_of(column[0] * quarter, quarter), quarter)
    out[...] = full[:, at].astype(jnp.bfloat16)


def body(
    grid_latent,
    mesh_latent,
    edge_latent,
    edge_src,
    edge_dst,
    edge_w1,
    edge_b1,
    edge_w2,
    edge_b2,
    edge_gain,
    edge_shift,
    node_w1,
    node_b1,
    node_w2,
    node_b2,
    node_gain,
    node_shift,
):
    bands = math.prod(SIZES.values())
    feats = FEATS
    quarter = grid_latent.shape[1]
    width = quarter * feats
    nodes = mesh_latent.shape[0]
    row = lambda v: v.reshape(1, -1)

    picked = pick_rows(grid_latent, edge_src.reshape(-1))
    picked = picked.reshape(bands * feats, -1, quarter)
    arrived = lax.all_to_all(picked, ("z", "core", "feat", "y"), 0, 0, tiled=True)

    edges = edge_latent.reshape(-1, width)
    targets = edge_dst.reshape(-1)
    slots = targets.shape[0]
    tiles = bands // GROUP
    live = jnp.any((targets < nodes).reshape(tiles, -1), 1).astype(jnp.int32)
    mesh_rows = lax.all_gather(mesh_latent, "feat", axis=1, tiled=True)

    pre, node_pre = pl.pallas_call(
        early_kernel,
        out_shape=[
            jax.ShapeDtypeStruct((slots, width), jnp.float32),
            jax.ShapeDtypeStruct((nodes, width), jnp.float32),
        ],
        in_specs=[SMEM] + [VMEM] * 7,
        out_specs=[VMEM] * 2,
        cost_estimate=pl.CostEstimate(
            flops=2 * slots * width * width * 2, bytes_accessed=12 << 20, transcendentals=0
        ),
        compiler_params=pltpu.CompilerParams(vmem_limit_bytes=16 << 20),
        name="early",
    )(live, edges, targets.reshape(-1, 1), mesh_rows, edge_w1, row(edge_b1), node_w1, row(node_b1))

    rows = slots // tiles
    first, second = pl.pallas_call(
        late_kernel,
        out_shape=[pltpu.VMEM((nodes // 2, width), jnp.bfloat16)] * 2,
        in_specs=[SMEM, VMEM, HBM, HBM] + [VMEM] * 6,
        out_specs=[VMEM] * 2,
        scratch_shapes=[
            pltpu.VMEM((tiles, rows, width), jnp.bfloat16),
            pltpu.VMEM((tiles, rows, width), jnp.float32),
            pltpu.VMEM((tiles, rows, width), jnp.float32),
            pltpu.VMEM((nodes, width), jnp.float32),
            pltpu.SemaphoreType.DMA((2, tiles)),
        ],
        cost_estimate=pl.CostEstimate(
            flops=2 * slots * width * width * 2, bytes_accessed=12 << 20, transcendentals=0
        ),
        compiler_params=pltpu.CompilerParams(vmem_limit_bytes=20 << 20),
        name="late",
    )(
        live,
        in_vmem(arrived),
        in_hbm(edges),
        in_hbm(pre),
        targets.reshape(tiles, 1, -1),
        in_vmem(edge_w1[width : 2 * width]),
        in_vmem(edge_w2),
        row(edge_b2),
        row(edge_gain),
        row(edge_shift),
    )

    pairing = [(i, i ^ 1) for i in range(feats)]
    crossing = [(i, feats - 1 - i) for i in range(feats)]
    first_got = lax.ppermute(first, "feat", pairing)
    second_got = lax.ppermute(second, "feat", crossing)
    add = lambda u, v: (u.astype(jnp.float32) + v.astype(jnp.float32)).astype(jnp.bfloat16)
    first = add(first, first_got)
    second = add(second, second_got)
    first_got = lax.ppermute(first, "feat", crossing)
    second_got = lax.ppermute(second, "feat", pairing)
    column = jnp.full((1,), lax.axis_index("feat"), jnp.int32)
    return pl.pallas_call(
        node_kernel,
        out_shape=jax.ShapeDtypeStruct((nodes, quarter), jnp.bfloat16),
        in_specs=[SMEM] + [VMEM] * 4 + [HBM] + [VMEM] * 5,
        out_specs=VMEM,
        scratch_shapes=[
            pltpu.VMEM((nodes, width), jnp.float32),
            pltpu.VMEM((nodes, width), jnp.float32),
            pltpu.SemaphoreType.DMA,
        ],
        compiler_params=pltpu.CompilerParams(vmem_limit_bytes=8 << 20),
        name="node",
    )(
        column,
        first,
        first_got,
        second,
        second_got,
        in_hbm(node_pre),
        mesh_rows,
        jnp.concatenate([node_w1[width:], node_w2], 0),
        row(node_b2),
        row(node_gain),
        row(node_shift),
    )


def solution(mesh):
    parts = jax.sharding.Mesh(
        mesh.devices.reshape(*SIZES.values(), FEATS), BAND + ("feat",), axis_types=(AUTO,) * 4
    )
    placed = (
        P(BAND, "feat"),
        P(BAND, "feat"),
        P(BAND, "feat", None, None),
        P(BAND, None),
        P(BAND, "feat", None),
    ) + (P(),) * 12
    return jax.shard_map(
        body, mesh=parts, in_specs=placed, out_specs=P(BAND, "feat"), check_vma=False
    )
```
